256 devices in a mesh: chan: 4 (over z_hi), pulse: 32 (over x, y, core), range: 2 (over z_lo).
Axes of the slice: x: 4, y: 4, z: 8 (z_hi: 4, z_lo: 2; z = z_hi * 2 + z_lo), core: 2. Of those that a mesh axis runs over, the one named last changes fastest.
Arguments:
- signal: bfloat16 [2, 64, 256, 8192], P(None, 'chan', 'pulse', 'range'), may hold values from -6 to 6
- steering: bfloat16 [2, 32, 64], replicated, may hold values from -0.5 to 0.5
- spectrum: float32 [2, 8192], replicated, may hold values from -6 to 6
Outputs:
- detection: float32 [32, 256, 8192], P('chan', 'pulse', 'range')
The draws below stay inside these ranges and needn't reach their ends.
All inputs are finite; a program needn't handle non-finite values.
Results may differ from the reference program's by a relative error of at most 0.0087.
Values may be sent and summed in bfloat16 or wider, within the bound.
A program may use at most 64 MiB of HBM per device.

```python
import math
import jax
import jax.numpy as jnp
from jax import lax

CH = 64
BEAMS = 32
GUARD = 4
TRAIN = 16
PULSES = 256
RANGE = 8192


def block_levels(own_key, shape, pieces, low, top_value):
    loudness, own = 1.0, jax.random.fold_in(own_key, 6)
    for position, blocks in pieces:
        draws = jnp.exp(jax.random.uniform(jax.random.fold_in(own, position), (blocks,), jnp.float32, low / len(pieces), top_value / len(pieces)))
        loudness = loudness * jnp.repeat(draws, shape[position] // blocks).reshape([-1 if axis == position else 1 for axis in range(len(shape))])
    return loudness


def scatter_about(stream_key, extent, width, reach, split=(), held_as=jnp.bfloat16):
    entries = jax.random.normal(stream_key, extent, jnp.float32) * width
    if len(split) > 0:
        entries = block_levels(stream_key, extent, split, -0.22, 0.18) * entries
    return jnp.clip(entries, min=-reach, max=reach).astype(held_as)


def setup_inputs(seed: int = 0) -> dict:
    splits = jax.random.split(jax.random.key(seed), 4)
    return {
        "signal": scatter_about(splits[0], (2, CH, PULSES, RANGE), 1.0, 6.0, ((1, 4), (2, 32), (3, 2))),
        "steering": scatter_about(splits[1], (2, BEAMS, CH), (2 * CH) ** -0.5, 0.5),
        "spectrum": scatter_about(splits[2], (2, RANGE), 1.0, 6.0, (), jnp.float32),
    }


NOISE_FLOOR = 0.25

def doppler_tables(pulse_count):
    row_ids = lax.broadcasted_iota(jnp.int32, (pulse_count, pulse_count), 0)
    col_ids = lax.broadcasted_iota(jnp.int32, (pulse_count, pulse_count), 1)
    phase_angle = (row_ids * col_ids % pulse_count).astype(jnp.float32) * (2.0 * math.pi / pulse_count)
    norm_scale = 1.0 / math.sqrt(pulse_count)
    table_real = (jnp.cos(phase_angle) * norm_scale).astype(jnp.bfloat16)
    table_imag = (-jnp.sin(phase_angle) * norm_scale).astype(jnp.bfloat16)
    return (table_real, table_imag)

def reference(signal, steering, spectrum):
    w_real = steering[0]
    w_imag = steering[1]
    stacked = jnp.concatenate([jnp.concatenate([w_real, -w_imag], 1), jnp.concatenate([w_imag, w_real], 1)], 0)
    flat_signal = signal.reshape(2 * CH, PULSES * RANGE)
    beam_data = jnp.dot(stacked, flat_signal, preferred_element_type=jnp.float32).astype(jnp.bfloat16)
    beam_data = beam_data.reshape(2, BEAMS, PULSES, RANGE)
    response = lax.complex(spectrum[0], spectrum[1])
    dop_real, dop_imag = doppler_tables(PULSES)
    halo_width = GUARD + TRAIN

    def one_beam(beam_slab):
        line_field = lax.complex(beam_slab[0].astype(jnp.float32), beam_slab[1].astype(jnp.float32))
        compressed = jnp.fft.ifft(jnp.fft.fft(line_field, axis=-1) * response, axis=-1)
        comp_real = jnp.real(compressed).astype(jnp.bfloat16)
        comp_imag = jnp.imag(compressed).astype(jnp.bfloat16)
        mixed_real = jnp.dot(dop_real, comp_real, preferred_element_type=jnp.float32) - jnp.dot(dop_imag, comp_imag, preferred_element_type=jnp.float32)
        mixed_imag = jnp.dot(dop_real, comp_imag, preferred_element_type=jnp.float32) + jnp.dot(dop_imag, comp_real, preferred_element_type=jnp.float32)
        power_map = mixed_real * mixed_real + mixed_imag * mixed_imag
        padded = jnp.pad(power_map, ((0, 0), (halo_width, halo_width)))
        window_sum = jnp.zeros_like(power_map)
        for offset in range(1, TRAIN + 1):
            left_start = halo_width - GUARD - offset
            right_start = halo_width + GUARD + offset
            window_sum = window_sum + padded[:, left_start:left_start + RANGE] + padded[:, right_start:right_start + RANGE]
        noise_level = window_sum / (2.0 * TRAIN)
        return power_map / (noise_level + NOISE_FLOOR)
    return lax.map(one_beam, jnp.transpose(beam_data, (1, 0, 2, 3)))
```

```python
import math

import jax
import jax.numpy as jnp
import numpy as np
from jax import lax
from jax.experimental import pallas as pl
from jax.experimental.pallas import tpu as pltpu
from jax.sharding import PartitionSpec as P

F32, BF16 = jnp.float32, jnp.bfloat16
MESH = pl.DeviceIdType.MESH
GUARD, TRAIN, NOISE_FLOOR = 4, 16, 0.25
NZ, NQ = 8, 32
HOPS = (4, 3, -3, 2, -2, 1, -1)
GROUPS = (2, 1, 3, 0)


def times(v, angle_num, period, sign):
    k = angle_num % period
    if k == 0:
        return v
    re, im = v
    if 4 * k == period:
        return (-im, re) if sign > 0 else (im, -re)
    if 2 * k == period:
        return (-re, -im)
    if 4 * k == 3 * period:
        return (im, -re) if sign > 0 else (-im, re)
    c = math.cos(2 * math.pi * k / period)
    s = sign * math.sin(2 * math.pi * k / period)
    return (re * c - im * s, re * s + im * c)


def dft(xs, sign):
    n = len(xs)
    if n == 1:
        return xs
    even, odd = dft(xs[0::2], sign), dft(xs[1::2], sign)
    odd = [times(v, k, n, sign) for k, v in enumerate(odd)]
    plus = [(a[0] + b[0], a[1] + b[1]) for a, b in zip(even, odd)]
    minus = [(a[0] - b[0], a[1] - b[1]) for a, b in zip(even, odd)]
    return plus + minus


def pair(x):
    x = x.astype(F32)
    return (x[:8], x[8:])


def joined(v):
    return jnp.concatenate(v, axis=0)


def lane_tables():
    n = np.arange(128)
    ang = 2 * np.pi * (np.outer(n, n) % 128) / 128
    c, s = np.cos(ang), np.sin(ang)
    ahead = np.block([[c, -s], [s, c]])
    back = np.block([[c, s], [-s, c]])
    k1 = (np.arange(8)[:, None] + 8 * np.arange(8)[None, :]).reshape(-1)
    turn = 2 * np.pi * np.outer(k1, n) / 8192
    twist = np.stack([np.cos(turn), -np.sin(turn)])
    return np.stack([ahead, back]), twist


def band_table():
    gap = np.abs(np.arange(512)[:, None] - (128 + np.arange(256)[None, :]))
    return ((gap > GUARD) & (gap <= GUARD + TRAIN)).astype(np.float32)


def spread(rows):
    return jnp.broadcast_to(rows[:, None, :], (8, 8, 128)).reshape(64, 128)


def zdev(z):
    return {"chan": z // 2, "range": lax.rem(z, 2)}


def kernel(
    sig, w, resp, lanes, twist, band, out,
    wide, send, recv, beams, mid, mid2, lhs, prod, comp, crossed, cols, dmid, power, rows, halo, win, noise, turned,
    ss1, rs1, ss2, rs2, ss3, rs3, ss4, rs4, ss5, rs5,
):
    c, q, r = lax.axis_index("chan"), lax.axis_index("pulse"), lax.axis_index("range")
    me = c * 2 + r
    bar = pltpu.get_barrier_semaphore()
    for d in range(1, NZ):
        pl.semaphore_signal(bar, inc=1, device_id=zdev(lax.rem(me + d, NZ)), device_id_type=MESH)

    def greet(d, carry):
        pl.semaphore_signal(bar, inc=1, device_id={"pulse": lax.rem(q + d, NQ)}, device_id_type=MESH)
        return carry

    lax.fori_loop(1, NQ, greet, 0)

    def widen(t, carry):
        x = sig[:, :, :, pl.ds(pl.multiple_of(t * 128, 128), 128)].astype(F32)
        wide[t] = x.reshape(256, 128)
        return carry

    lax.fori_loop(0, 32, widen, 0)

    def hop(k):
        t = lax.rem(me + HOPS[k] + NZ, NZ)
        return t, pltpu.make_async_remote_copy(
            src_ref=send.at[t], dst_ref=recv.at[me], send_sem=ss1.at[k], recv_sem=rs1.at[k],
            device_id=zdev(t), device_id_type=MESH,
        )

    def take_pulse(j):
        def one(t, carry):
            send[j, t] = wide[t, pl.ds(j, 32, stride=8), :].astype(BF16)
            return carry

        lax.fori_loop(0, 32, one, 0, unroll=4)

    for k in range(7):
        t, copy = hop(k)
        take_pulse(t)
        if k == 0:
            pl.semaphore_wait(bar, NZ - 1 + NQ - 1)
        copy.start()

    def own(t, carry):
        recv[me, t] = wide[t, pl.ds(me, 32, stride=8), :].astype(BF16)
        return carry

    lax.fori_loop(0, 32, own, 0, unroll=4)
    for k in range(7):
        hop(k)[1].wait()

    for half in range(2):

        def form(i, carry, half=half):
            cols2 = [jnp.concatenate([recv[2 * cc + half, 2 * i + e] for cc in range(4)], axis=0) for e in range(2)]
            got = jnp.dot(w[...], jnp.concatenate(cols2, axis=1), preferred_element_type=F32).astype(BF16)
            for e in range(2):
                beams[half * 32 + 2 * i + e] = got[:, e * 128 : (e + 1) * 128].reshape(4, 16, 128)
            return carry

        lax.fori_loop(0, 16, form, 0)

    def cross(g, d):
        t = lax.rem(q + d, NQ)
        return pltpu.make_async_remote_copy(
            src_ref=comp.at[g, :, t], dst_ref=crossed.at[g, :, q], send_sem=ss2.at[g], recv_sem=rs2.at[g],
            device_id={"pulse": t}, device_id_type=MESH,
        )

    def filter_group(g):
        for b in range(8):
            ys = dft([pair(beams[8 * a + b, g]) for a in range(8)], -1)
            for ka in range(8):
                mid[b * 8 + ka] = joined(times(ys[ka], b * ka, 64, -1))
        for ka in range(8):
            xs = dft([pair(mid[b * 8 + ka]) for b in range(8)], -1)
            tr, ti = twist[0, ka * 8 : ka * 8 + 8, :], twist[1, ka * 8 : ka * 8 + 8, :]
            tr, ti = spread(tr), spread(ti)
            re = jnp.concatenate([v[0] for v in xs], axis=0)
            im = jnp.concatenate([v[1] for v in xs], axis=0)
            lhs[ka * 64 : ka * 64 + 64, 0:128] = (re * tr - im * ti).astype(BF16)
            lhs[ka * 64 : ka * 64 + 64, 128:256] = (re * ti + im * tr).astype(BF16)
        prod[...] = jnp.dot(lhs[...], lanes[0], preferred_element_type=F32)
        for ka in range(8):
            hr, hi = spread(resp[0, ka * 8 : ka * 8 + 8, :]), spread(resp[1, ka * 8 : ka * 8 + 8, :])
            re, im = prod[ka * 64 : ka * 64 + 64, 0:128], prod[ka * 64 : ka * 64 + 64, 128:256]
            lhs[ka * 64 : ka * 64 + 64, 0:128] = (re * hr - im * hi).astype(BF16)
            lhs[ka * 64 : ka * 64 + 64, 128:256] = (re * hi + im * hr).astype(BF16)
        prod[...] = jnp.dot(lhs[...], lanes[1], preferred_element_type=F32)
        for ka in range(8):
            tr, ti = spread(twist[0, ka * 8 : ka * 8 + 8, :]), spread(twist[1, ka * 8 : ka * 8 + 8, :])
            re, im = prod[ka * 64 : ka * 64 + 64, 0:128], prod[ka * 64 : ka * 64 + 64, 128:256]
            re, im = re * tr + im * ti, im * tr - re * ti
            ys = dft([(re[8 * kb : 8 * kb + 8], im[8 * kb : 8 * kb + 8]) for kb in range(8)], 1)
            for b in range(8):
                mid2[b * 8 + ka] = joined(times(ys[b], b * ka, 64, 1))
        for b in range(8):
            xs = dft([pair(mid2[b * 8 + ka]) for ka in range(8)], 1)
            for a in range(8):
                n1 = 8 * a + b
                comp[g, n1 // 32, n1 % 32] = joined(xs[a]).astype(BF16)

    def group(step):
        offset = jnp.where(step == 0, 2, jnp.where(step == 1, 1, jnp.where(step == 2, 3, 0)))
        return lax.rem(c + offset, 4)

    def each_group(step, carry):
        g = group(step)
        filter_group(g)

        def start(d, cc):
            cross(g, d).start()
            return cc

        lax.fori_loop(1, NQ, start, 0)
        for rr in range(2):
            crossed[g, rr, q] = comp[g, rr, q]
        return carry

    lax.fori_loop(0, 4, each_group, 0)

    def to_owner(k, g, rr):
        return pltpu.make_async_remote_copy(
            src_ref=crossed.at[g, rr], dst_ref=cols.at[me], send_sem=ss3.at[k], recv_sem=rs3.at[k],
            device_id={"chan": g, "range": rr}, device_id_type=MESH,
        )

    moves = []
    for step, offset in enumerate(GROUPS):
        g = lax.rem(c + offset, 4)
        for e in range(2):
            if offset == 0 and e == 0:
                continue
            moves.append((len(moves), step, g, lax.rem(r + e, 2)))
    seen = -1
    for k, step, g, rr in moves:
        if step != seen:
            whole = crossed.at[g, :, pl.ds(0, NQ - 1)]
            pltpu.make_async_copy(whole, whole, rs2.at[g]).wait()
            seen = step
        to_owner(k, g, rr).start()

    def keep(t, carry):
        cols[me, t] = crossed[c, r, t]
        return carry

    lax.fori_loop(0, NQ, keep, 0, unroll=4)
    for k, step, g, rr in moves:
        to_owner(k, g, rr).wait()
    for g in range(4):
        whole = comp.at[g, :, pl.ds(0, NQ - 1)]
        pltpu.make_async_copy(whole, whole, ss2.at[g]).wait()

    for b in range(16):
        ps = [16 * a + b for a in range(16)]
        ys = dft([pair(cols[p % 8, p // 8]) for p in ps], -1)
        for fa in range(16):
            dmid[b * 16 + fa] = joined(times(ys[fa], b * fa, 256, -1))
    for fa in range(16):
        xs = dft([pair(dmid[b * 16 + fa]) for b in range(16)], -1)
        for fb in range(16):
            re, im = xs[fb]
            power[fa + 16 * fb] = ((re * re + im * im) * (1.0 / 256)).astype(BF16)

    def to_bins(d):
        t = lax.rem(q + d, NQ)
        return pltpu.make_async_remote_copy(
            src_ref=power.at[pl.ds(t * 8, 8)], dst_ref=rows.at[q], send_sem=ss4.at[d], recv_sem=rs4.at[d],
            device_id={"pulse": t}, device_id_type=MESH,
        )

    def start_bins(d, carry):
        to_bins(d).start()
        return carry

    def wait_bins(d, carry):
        to_bins(d).wait()
        return carry

    lax.fori_loop(1, NQ, start_bins, 0)
    for f in range(8):
        rows[q, f] = power[q * 8 + f]
    lax.fori_loop(1, NQ, wait_bins, 0)
    edge = pltpu.make_async_remote_copy(
        src_ref=rows.at[(1 - r) * (NQ - 1)], dst_ref=halo, send_sem=ss5, recv_sem=rs5,
        device_id={"range": 1 - r}, device_id_type=MESH,
    )
    edge.start()

    def flat(x):
        return x.astype(F32).reshape(64, 128).astype(BF16)

    def place(i, tile, x):
        win[i, :, tile * 128 : (tile + 1) * 128] = x

    for i in range(16):
        x0, x1 = flat(rows[2 * i]), flat(rows[2 * i + 1])
        place(i, 1, x0)
        place(i, 2, x1)
        if i > 0:
            place(i - 1, 3, x0)
        if i < 15:
            place(i + 1, 0, x1)
    edge.wait()
    beside = halo[...].astype(F32).reshape(64, 128)
    right = r.astype(F32)
    place(0, 0, (beside * right).astype(BF16))
    place(15, 3, (beside * (1.0 - right)).astype(BF16))
    noise[...] = jnp.dot(win[...].reshape(1024, 512), band[...], preferred_element_type=F32)
    for i in range(16):
        for e in range(2):
            level = noise[i * 64 : (i + 1) * 64, e * 128 : (e + 1) * 128] * (1.0 / (2 * TRAIN)) + NOISE_FLOOR
            got = rows[2 * i + e].astype(F32).reshape(64, 128) / level
            at = (2 * i + e) * 128
            for f in range(8):
                turned[2 * i + e, pl.ds(f, 8, stride=8), :] = got[f * 8 : f * 8 + 8]
            out[:, at : at + 128] = turned[2 * i + e]


def shards(signal, steering, spectrum):
    lanes, twist = lane_tables()
    wr, wi = (x.reshape(4, 8, 4, 16).transpose(0, 1, 2, 3) for x in (steering[0], steering[1]))
    top = jnp.stack([wr, -wi], axis=3)
    low = jnp.stack([wi, wr], axis=3)
    w = jnp.stack([top, low], axis=1).reshape(64, 128)
    resp = spectrum.reshape(2, 128, 8, 8).transpose(0, 3, 2, 1).reshape(2, 64, 128) * (1.0 / 8192)
    vm = pl.BlockSpec(memory_space=pltpu.VMEM)
    scratch = [
        pltpu.VMEM((32, 256, 128), F32),
        pltpu.VMEM((8, 32, 32, 128), BF16),
        pltpu.VMEM((8, 32, 32, 128), BF16),
        pltpu.VMEM((64, 4, 16, 128), BF16),
        pltpu.VMEM((64, 16, 128), F32),
        pltpu.VMEM((64, 16, 128), F32),
        pltpu.VMEM((512, 256), BF16),
        pltpu.VMEM((512, 256), F32),
        pltpu.VMEM((4, 2, 32, 16, 128), BF16),
        pltpu.VMEM((4, 2, 32, 16, 128), BF16),
        pltpu.VMEM((8, 32, 16, 128), BF16),
        pltpu.VMEM((256, 16, 128), F32),
        pltpu.VMEM((256, 8, 128), BF16),
        pltpu.VMEM((32, 8, 8, 128), BF16),
        pltpu.VMEM((8, 8, 128), BF16),
        pltpu.VMEM((16, 64, 512), BF16),
        pltpu.VMEM((1024, 256), F32),
        pltpu.VMEM((32, 64, 128), F32),
        pltpu.SemaphoreType.DMA((7,)), pltpu.SemaphoreType.DMA((7,)),
        pltpu.SemaphoreType.DMA((4,)), pltpu.SemaphoreType.DMA((4,)),
        pltpu.SemaphoreType.DMA((7,)), pltpu.SemaphoreType.DMA((7,)),
        pltpu.SemaphoreType.DMA((32,)), pltpu.SemaphoreType.DMA((32,)),
        pltpu.SemaphoreType.DMA, pltpu.SemaphoreType.DMA,
    ]
    got = pl.pallas_call(
        kernel,
        out_shape=jax.ShapeDtypeStruct((64, 4096), F32),
        in_specs=[vm] * 6,
        out_specs=vm,
        scratch_shapes=scratch,
        compiler_params=pltpu.CompilerParams(collective_id=0, has_side_effects=True, vmem_limit_bytes=60 * 2**20),
        name="radar",
    )(
        signal, w, resp, jnp.asarray(lanes, BF16), jnp.asarray(twist, F32), jnp.asarray(band_table(), BF16),
    )
    return got.reshape(8, 8, 4096)


def solution(mesh):
    return jax.shard_map(
        shards,
        mesh=mesh,
        in_specs=(P(None, "chan", "pulse", "range"), P(), P()),
        out_specs=P("chan", "pulse", "range"),
        check_vma=False,
    )
```

```python
import math

import jax
import jax.numpy as jnp
import numpy as np
from jax import lax
from jax.experimental import pallas as pl
from jax.experimental.pallas import tpu as pltpu
from jax.sharding import PartitionSpec as P

F32, BF16 = jnp.float32, jnp.bfloat16
MESH = pl.DeviceIdType.MESH
GUARD, TRAIN, NOISE_FLOOR = 4, 16, 0.25
NZ, NQ = 8, 32
HOPS = (4, 3, -3, 2, -2, 1, -1)
CHUNKS = 4
PEERS = sorted(
    ((x, y, k) for x in range(4) for y in range(4) for k in range(2) if x + y + k),
    key=lambda d: -(min(d[0], 4 - d[0]) + min(d[1], 4 - d[1])),
)


def times(v, angle_num, period, sign):
    k = angle_num % period
    if k == 0:
        return v
    re, im = v
    if 4 * k == period:
        return (-im, re) if sign > 0 else (im, -re)
    if 2 * k == period:
        return (-re, -im)
    if 4 * k == 3 * period:
        return (im, -re) if sign > 0 else (-im, re)
    c = math.cos(2 * math.pi * k / period)
    s = sign * math.sin(2 * math.pi * k / period)
    return (re * c - im * s, re * s + im * c)


def dft(xs, sign):
    n = len(xs)
    if n == 1:
        return xs
    even, odd = dft(xs[0::2], sign), dft(xs[1::2], sign)
    odd = [times(v, k, n, sign) for k, v in enumerate(odd)]
    plus = [(a[0] + b[0], a[1] + b[1]) for a, b in zip(even, odd)]
    minus = [(a[0] - b[0], a[1] - b[1]) for a, b in zip(even, odd)]
    return plus + minus


def pair(x):
    x = x.astype(F32)
    return (x[:8], x[8:])


def joined(v):
    return jnp.concatenate(v, axis=0)


def lane_tables():
    n = np.arange(128)
    k2 = 2 * (n % 64) + n // 64
    ang = 2 * np.pi * (np.outer(n, k2) % 128) / 128
    c, s = np.cos(ang), np.sin(ang)
    ahead = np.block([[c, -s], [s, c]])
    back = np.block([[c.T, s.T], [-s.T, c.T]])
    k1 = (np.arange(8)[:, None] + 8 * np.arange(8)[None, :]).reshape(-1)
    turn = 2 * np.pi * np.outer(k1, n) / 8192
    twist = np.stack([np.cos(turn), -np.sin(turn)])
    return np.stack([ahead, back]), twist


def spread(rows):
    return jnp.broadcast_to(rows[:, None, :], (8, 8, 128)).reshape(64, 128)


def zdev(z):
    return {"chan": z // 2, "range": lax.rem(z, 2)}


def qpeer(q, d):
    x, y, k = q // 8, lax.rem(q // 2, 4), lax.rem(q, 2)
    return lax.rem(x + d[0], 4) * 8 + lax.rem(y + d[1], 4) * 2 + lax.rem(k + d[2], 2)


def kernel(
    sig_hbm, steer_hbm, spec_hbm, lanes_hbm, twist_hbm, out,
    sig, steer, spec, lanes, twist, wmat, rowed, turned_resp, resp, tw, band,
    wide, send, recv, formed, mid, mid2, lhs, prod, comp, crossed, early, cols, dmid, power, rows, halo, win, noise, turned,
    loads, ss1, rs1, ss2, rs2, ss3, rs3, ss4, rs4, ss5, rs5, ss6, rs6,
):
    c, q, r = lax.axis_index("chan"), lax.axis_index("pulse"), lax.axis_index("range")
    me = c * 2 + r
    bar = pltpu.get_barrier_semaphore()
    for d in range(1, NZ):
        pl.semaphore_signal(bar, inc=1, device_id=zdev(lax.rem(me + d, NZ)), device_id_type=MESH)

    def greet(d, carry):
        pl.semaphore_signal(bar, inc=1, device_id={"pulse": lax.rem(q + d, NQ)}, device_id_type=MESH)
        return carry

    lax.fori_loop(1, NQ, greet, 0)
    fetched = [
        pltpu.make_async_copy(a, b, loads.at[i])
        for i, (a, b) in enumerate(
            [(sig_hbm, sig), (steer_hbm, steer), (spec_hbm, spec), (lanes_hbm, lanes), (twist_hbm, twist)]
        )
    ]
    for copy in fetched:
        copy.start()
    fetched[0].wait()

    def widen(t, carry):
        x = sig[:, :, :, pl.ds(pl.multiple_of(t * 128, 128), 128)].astype(F32)
        wide[t] = x.reshape(256, 128)
        return carry

    lax.fori_loop(0, 32, widen, 0, unroll=2)
    per = 8 // CHUNKS

    def take_pulse(j, part, into, at):
        for b in range(part * per, (part + 1) * per):
            for a in range(4):
                into[at, b, a] = wide[8 * a + b, pl.ds(j, 32, stride=8), :].astype(BF16)

    def hop(k, part):
        t = lax.rem(me + HOPS[k] + NZ, NZ)
        mine = pl.ds(part * per, per)
        return t, pltpu.make_async_remote_copy(
            src_ref=send.at[t, mine], dst_ref=recv.at[me, mine], send_sem=ss1.at[k, part], recv_sem=rs1.at[k, part],
            device_id=zdev(t), device_id_type=MESH,
        )

    for part in range(CHUNKS):
        for k in range(7):
            t, copy = hop(k, part)
            take_pulse(t, part, send, t)
            if k == 0 and part == 0:
                pl.semaphore_wait(bar, NZ - 1 + NQ - 1)
            copy.start()
    for part in range(CHUNKS):
        take_pulse(me, part, recv, me)

    for copy in fetched[1:]:
        copy.wait()
    wr, wi = steer[0].astype(F32), steer[1].astype(F32)
    wmat[0:32] = jnp.concatenate([wr, -wi], axis=1).astype(BF16)
    wmat[32:64] = jnp.concatenate([wi, wr], axis=1).astype(BF16)
    for i in range(2):
        for m in range(64):
            rowed[m : m + 1] = spec[i : i + 1, m * 128 : (m + 1) * 128]
        a = rowed[...] * (1.0 / 8192)
        both = jnp.concatenate([a, jnp.concatenate([a[:, 64:], a[:, :64]], axis=1)], axis=0)
        turned_resp[...] = jnp.transpose(both)
        for ka in range(8):
            resp[i, ka * 64 : ka * 64 + 64] = spread(turned_resp[pl.ds(ka, 8, stride=8), :])
            tw[i, ka * 64 : ka * 64 + 64] = spread(twist[i, ka * 8 : ka * 8 + 8])

    def make_band(i, carry):
        row = lax.broadcasted_iota(jnp.int32, (64, 256), 0) + i * 64
        gap = jnp.abs(row - 128 - lax.broadcasted_iota(jnp.int32, (64, 256), 1))
        ones = jnp.where((gap > GUARD) & (gap <= GUARD + TRAIN), 1.0, 0.0)
        band[pl.ds(pl.multiple_of(i * 64, 64), 64), :] = ones.astype(BF16)
        return carry

    lax.fori_loop(0, 8, make_band, 0)
    win[0, :, 0:128] = jnp.zeros((64, 128), BF16)
    win[15, :, 384:512] = jnp.zeros((64, 128), BF16)

    def front(b):
        now = b % 2
        for half in range(2):
            for a in (0, 2):
                blocks = []
                for e in range(2):
                    tiles = [recv[2 * cc + half, b, a + e] for cc in range(4)]
                    blocks.append(jnp.concatenate([t[:16] for t in tiles] + [t[16:] for t in tiles], axis=0))
                got = jnp.dot(wmat[...], jnp.concatenate(blocks, axis=1), preferred_element_type=F32)
                got = got.astype(BF16).astype(F32)
                for e in range(2):
                    formed[now, half * 4 + a + e] = got[:, e * 128 : (e + 1) * 128]
        for g in range(4):
            xs = [(formed[now, a, 8 * g : 8 * g + 8], formed[now, a, 32 + 8 * g : 40 + 8 * g]) for a in range(8)]
            ys = dft(xs, -1)
            for ka in range(8):
                mid[g, b * 8 + ka] = joined(times(ys[ka], b * ka, 64, -1))

    for part in range(CHUNKS):
        for k in range(7):
            hop(k, part)[1].wait_recv()
        for b in range(part * per, (part + 1) * per):
            front(b)

    def filter_group(g):
        for ka in range(8):
            here = slice(ka * 64, ka * 64 + 64)
            xs = dft([pair(mid[g, b * 8 + ka]) for b in range(8)], -1)
            tr, ti = tw[0, here], tw[1, here]
            re = jnp.concatenate([v[0] for v in xs], axis=0)
            im = jnp.concatenate([v[1] for v in xs], axis=0)
            lhs[here, 0:128] = (re * tr - im * ti).astype(BF16)
            lhs[here, 128:256] = (re * ti + im * tr).astype(BF16)
        prod[...] = jnp.dot(lhs[...], lanes[0], preferred_element_type=F32)
        for ka in range(8):
            here = slice(ka * 64, ka * 64 + 64)
            hr, hi = resp[0, here], resp[1, here]
            re, im = prod[here, 0:128], prod[here, 128:256]
            lhs[here, 0:128] = (re * hr - im * hi).astype(BF16)
            lhs[here, 128:256] = (re * hi + im * hr).astype(BF16)
        prod[...] = jnp.dot(lhs[...], lanes[1], preferred_element_type=F32)
        for ka in range(8):
            here = slice(ka * 64, ka * 64 + 64)
            tr, ti = tw[0, here], tw[1, here]
            re, im = prod[here, 0:128], prod[here, 128:256]
            re, im = re * tr + im * ti, im * tr - re * ti
            ys = dft([(re[8 * kb : 8 * kb + 8], im[8 * kb : 8 * kb + 8]) for kb in range(8)], 1)
            for b in range(8):
                mid2[b * 8 + ka] = joined(times(ys[b], b * ka, 64, 1))
        for b in range(8):
            xs = dft([pair(mid2[b * 8 + ka]) for ka in range(8)], 1)
            for a in range(8):
                n1 = 8 * a + b
                comp[g, n1 // 32, n1 % 32] = joined(xs[a]).astype(BF16)

    far = lax.rem(c + 2, 4)

    def far_copy(e):
        rr = lax.rem(r + e, 2)
        return pltpu.make_async_remote_copy(
            src_ref=comp.at[far, rr], dst_ref=early.at[r], send_sem=ss3.at[e], recv_sem=rs3.at[e],
            device_id={"chan": far, "range": rr}, device_id_type=MESH,
        )

    filter_group(far)
    for e in range(2):
        far_copy(e).start()

    def cross(g, d):
        t = qpeer(q, d)
        return pltpu.make_async_remote_copy(
            src_ref=comp.at[g, :, t], dst_ref=crossed.at[g, :, q], send_sem=ss2.at[g], recv_sem=rs2.at[g],
            device_id={"pulse": t}, device_id_type=MESH,
        )

    def each_group(step, carry):
        g = lax.rem(c + jnp.where(step == 0, 1, jnp.where(step == 1, 3, 0)), 4)
        filter_group(g)
        for d in PEERS:
            cross(g, d).start()
        for rr in range(2):
            crossed[g, rr, q] = comp[g, rr, q]
        return carry

    lax.fori_loop(0, 3, each_group, 0)

    def to_owner(k, g, rr):
        return pltpu.make_async_remote_copy(
            src_ref=crossed.at[g, rr], dst_ref=cols.at[me], send_sem=ss3.at[k], recv_sem=rs3.at[k],
            device_id={"chan": g, "range": rr}, device_id_type=MESH,
        )

    moves = []
    for offset in (1, 3, 0):
        g = lax.rem(c + offset, 4)
        whole = crossed.at[g, :, pl.ds(0, NQ - 1)]
        pltpu.make_async_copy(whole, whole, rs2.at[g]).wait()
        for e in range(2):
            if offset or e:
                moves.append(to_owner(2 + len(moves), g, lax.rem(r + e, 2)))
                moves[-1].start()

    def forward(d):
        t = qpeer(q, d)
        return pltpu.make_async_remote_copy(
            src_ref=early.at[:, t], dst_ref=cols.at[pl.ds(2 * far, 2), q], send_sem=ss6, recv_sem=rs6,
            device_id={"pulse": t}, device_id_type=MESH,
        )

    for e in range(2):
        far_copy(e).wait()
    for d in PEERS:
        forward(d).start()
    for rr in range(2):
        cols[2 * far + rr, q] = early[rr, q]

    def keep(t, carry):
        cols[me, t] = crossed[c, r, t]
        return carry

    lax.fori_loop(0, NQ, keep, 0, unroll=4)
    for part in range(CHUNKS):
        for k in range(7):
            hop(k, part)[1].wait_send()
    for move in moves:
        move.wait()
    whole = early.at[:, pl.ds(0, NQ - 1)]
    pltpu.make_async_copy(whole, whole, rs6).wait()
    pltpu.make_async_copy(whole, whole, ss6).wait()
    for offset in (1, 3, 0):
        g = lax.rem(c + offset, 4)
        whole = comp.at[g, :, pl.ds(0, NQ - 1)]
        pltpu.make_async_copy(whole, whole, ss2.at[g]).wait()

    for b in range(16):
        ps = [16 * a + b for a in range(16)]
        ys = dft([pair(cols[p % 8, p // 8]) for p in ps], -1)
        for fa in range(16):
            dmid[b * 16 + fa] = joined(times(ys[fa], b * fa, 256, -1))
    for fa in range(16):
        xs = dft([pair(dmid[b * 16 + fa]) for b in range(16)], -1)
        for fb in range(16):
            re, im = xs[fb]
            power[fa + 16 * fb] = ((re * re + im * im) * (1.0 / 256)).astype(BF16)

    def to_bins(i):
        t = qpeer(q, PEERS[i])
        return pltpu.make_async_remote_copy(
            src_ref=power.at[pl.ds(t * 8, 8)], dst_ref=rows.at[q], send_sem=ss4.at[i], recv_sem=rs4.at[q],
            device_id={"pulse": t}, device_id_type=MESH,
        )

    def from_bins(s):
        return pltpu.make_async_remote_copy(
            src_ref=power.at[pl.ds(s * 8, 8)], dst_ref=rows.at[s], send_sem=ss4.at[0], recv_sem=rs4.at[s],
            device_id={"pulse": s}, device_id_type=MESH,
        )

    for i in range(NQ - 1):
        to_bins(i).start()
    rows[q] = power[pl.ds(q * 8, 8)]
    outer = (1 - r) * (NQ - 1)

    @pl.when(q != outer)
    def _():
        from_bins(outer).wait_recv()

    edge = pltpu.make_async_remote_copy(
        src_ref=rows.at[outer], dst_ref=halo, send_sem=ss5, recv_sem=rs5,
        device_id={"range": 1 - r}, device_id_type=MESH,
    )
    edge.start()

    def wait_bins(d, carry):
        s = lax.rem(q + d, NQ)

        @pl.when(s != outer)
        def _():
            from_bins(s).wait_recv()

        return carry

    lax.fori_loop(1, NQ, wait_bins, 0)

    def flat(x):
        return x.astype(F32).reshape(64, 128)

    def place(i, tile, x):
        win[i, :, tile * 128 : (tile + 1) * 128] = x

    for i in range(16):
        x0, x1 = flat(rows[2 * i]).astype(BF16), flat(rows[2 * i + 1]).astype(BF16)
        place(i, 1, x0)
        place(i, 2, x1)
        if i > 0:
            place(i - 1, 3, x0)
        if i < 15:
            place(i + 1, 0, x1)
    noise[...] = jnp.dot(win[...].reshape(1024, 512), band[...], preferred_element_type=F32)

    def detect(t, more):
        i, e = t // 2, t % 2
        level = noise[i * 64 : (i + 1) * 64, e * 128 : (e + 1) * 128] + more
        got = flat(rows[t]) / (level * (1.0 / (2 * TRAIN)) + NOISE_FLOOR)
        for f in range(8):
            turned[t, pl.ds(f, 8, stride=8), :] = got[f * 8 : f * 8 + 8]
        out[:, t * 128 : (t + 1) * 128] = turned[t].astype(out.dtype)

    for t in range(1, 31):
        detect(t, 0.0)
    edge.wait()
    beside, right = flat(halo[...]), r.astype(F32)
    low = jnp.dot((beside * right).astype(BF16), band[0:128, 0:128], preferred_element_type=F32)
    high = jnp.dot((beside * (1.0 - right)).astype(BF16), band[384:512, 128:256], preferred_element_type=F32)
    detect(0, low)
    detect(31, high)
    for i in range(NQ - 1):
        to_bins(i).wait_send()


def shards(signal, steering, spectrum):
    lanes, twist = lane_tables()
    dma = pltpu.SemaphoreType.DMA
    scratch = [
        pltpu.VMEM((2, 16, 8, 4096), BF16),
        pltpu.VMEM((2, 32, 64), BF16),
        pltpu.VMEM((2, 8192), F32),
        pltpu.VMEM((2, 256, 256), BF16),
        pltpu.VMEM((2, 64, 128), F32),
        pltpu.VMEM((64, 128), BF16),
        pltpu.VMEM((64, 128), F32),
        pltpu.VMEM((128, 128), F32),
        pltpu.VMEM((2, 512, 128), F32),
        pltpu.VMEM((2, 512, 128), F32),
        pltpu.VMEM((512, 256), BF16),
        pltpu.VMEM((32, 256, 128), F32),
        pltpu.VMEM((8, 8, 4, 32, 128), BF16),
        pltpu.VMEM((8, 8, 4, 32, 128), BF16),
        pltpu.VMEM((2, 8, 64, 128), F32),
        pltpu.VMEM((4, 64, 16, 128), F32),
        pltpu.VMEM((64, 16, 128), F32),
        pltpu.VMEM((512, 256), BF16),
        pltpu.VMEM((512, 256), F32),
        pltpu.VMEM((4, 2, 32, 16, 128), BF16),
        pltpu.VMEM((4, 2, 32, 16, 128), BF16),
        pltpu.VMEM((2, 32, 16, 128), BF16),
        pltpu.VMEM((8, 32, 16, 128), BF16),
        pltpu.VMEM((256, 16, 128), F32),
        pltpu.VMEM((256, 8, 128), BF16),
        pltpu.VMEM((32, 8, 8, 128), BF16),
        pltpu.VMEM((8, 8, 128), BF16),
        pltpu.VMEM((16, 64, 512), BF16),
        pltpu.VMEM((1024, 256), F32),
        pltpu.VMEM((32, 64, 128), F32),
        dma((5,)),
        dma((7, CHUNKS)), dma((7, CHUNKS)),
        dma((4,)), dma((4,)),
        dma((7,)), dma((7,)),
        dma((32,)), dma((32,)),
        dma, dma,
        dma, dma,
    ]
    got = pl.pallas_call(
        kernel,
        out_shape=jax.ShapeDtypeStruct((64, 4096), BF16),
        in_specs=[pl.BlockSpec(memory_space=pl.ANY)] * 5,
        out_specs=pl.BlockSpec(memory_space=pltpu.VMEM),
        scratch_shapes=scratch,
        compiler_params=pltpu.CompilerParams(collective_id=0, has_side_effects=True, vmem_limit_bytes=60 * 2**20),
        name="radar",
    )(signal, steering, spectrum, jnp.asarray(lanes, BF16), jnp.asarray(twist, F32))
    return got.reshape(8, 8, 4096).astype(F32)


def solution(mesh):
    return jax.shard_map(
        shards,
        mesh=mesh,
        in_specs=(P(None, "chan", "pulse", "range"), P(), P()),
        out_specs=P("chan", "pulse", "range"),
        check_vma=False,
    )
```

```python
import math

import jax
import jax.numpy as jnp
import numpy as np
from jax import lax
from jax.experimental import pallas as pl
from jax.experimental.pallas import tpu as pltpu
from jax.sharding import PartitionSpec as P

F32, BF16 = jnp.float32, jnp.bfloat16
MESH = pl.DeviceIdType.MESH
GUARD, TRAIN, NOISE_FLOOR = 4, 16, 0.25
NZ, NQ = 8, 32
HOPS = (4, 3, -3, 2, -2, 1, -1)
GROUPS = (2, 1, 3, 0)
NEAR_LAST = (10, 6, 9, 11, 14, 2, 8, 5, 7, 13, 15, 1, 3, 4, 12)
CHUNKS = 4


def times(v, angle_num, period, sign):
    k = angle_num % period
    if k == 0:
        return v
    re, im = v
    if 4 * k == period:
        return (-im, re) if sign > 0 else (im, -re)
    if 2 * k == period:
        return (-re, -im)
    if 4 * k == 3 * period:
        return (im, -re) if sign > 0 else (-im, re)
    c = math.cos(2 * math.pi * k / period)
    s = sign * math.sin(2 * math.pi * k / period)
    return (re * c - im * s, re * s + im * c)


def dft(xs, sign):
    n = len(xs)
    if n == 1:
        return xs
    even, odd = dft(xs[0::2], sign), dft(xs[1::2], sign)
    odd = [times(v, k, n, sign) for k, v in enumerate(odd)]
    plus = [(a[0] + b[0], a[1] + b[1]) for a, b in zip(even, odd)]
    minus = [(a[0] - b[0], a[1] - b[1]) for a, b in zip(even, odd)]
    return plus + minus


def pair(x):
    x = x.astype(F32)
    return (x[:8], x[8:])


def joined(v):
    return jnp.concatenate(v, axis=0)


def lane_tables():
    n = np.arange(128)
    k2 = 2 * (n % 64) + n // 64
    ang = 2 * np.pi * (np.outer(n, k2) % 128) / 128
    c, s = np.cos(ang), np.sin(ang)
    ahead = np.block([[c, -s], [s, c]])
    back = np.block([[c.T, s.T], [-s.T, c.T]])
    k1 = (np.arange(8)[:, None] + 8 * np.arange(8)[None, :]).reshape(-1)
    turn = 2 * np.pi * np.outer(k1, n) / 8192
    twist = np.stack([np.cos(turn), -np.sin(turn)])
    return np.stack([ahead, back]), twist


def spread(rows):
    return jnp.broadcast_to(rows[:, None, :], (8, 8, 128)).reshape(64, 128)


def zdev(z):
    return {"chan": z // 2, "range": lax.rem(z, 2)}


def kernel(
    sig_hbm, steer_hbm, spec_hbm, lanes_hbm, twist_hbm, rows_hbm, halo,
    sig, steer, spec, lanes, twist, wmat, rowed, turned_resp, resp, tw,
    wide, send, recv, formed, mid, mid2, lhs, prod, comp, crossed, early, cols, dmid, power, rows,
    loads, parts, ss1, rs1, ss2, rs2, ss3, rs3, ss4, rs4, ss5, rs5, ss6, rs6, ss7, rs7, stores,
):
    c, q, r = lax.axis_index("chan"), lax.axis_index("pulse"), lax.axis_index("range")
    me = c * 2 + r
    bar = pltpu.get_barrier_semaphore()
    for d in range(1, NZ):
        pl.semaphore_signal(bar, inc=1, device_id=zdev(lax.rem(me + d, NZ)), device_id_type=MESH)

    def greet(d, carry):
        pl.semaphore_signal(bar, inc=1, device_id={"pulse": lax.rem(q + d, NQ)}, device_id_type=MESH)
        return carry

    lax.fori_loop(1, NQ, greet, 0)
    fetched = [
        pltpu.make_async_copy(a, b, loads.at[i])
        for i, (a, b) in enumerate(
            [(steer_hbm, steer), (spec_hbm, spec), (lanes_hbm, lanes), (twist_hbm, twist)]
        )
    ]
    per = 8 // CHUNKS

    def part_copy(part, a):
        at = (slice(None), slice(None), slice(None), pl.ds((8 * a + part * per) * 128, per * 128))
        return pltpu.make_async_copy(sig_hbm.at[at], sig.at[at], parts.at[part, a])

    for part in range(CHUNKS):
        for a in range(4):
            part_copy(part, a).start()
    for copy in fetched:
        copy.start()

    def widen(part):
        for a in range(4):
            part_copy(part, a).wait()
        for a in range(4):
            for b in range(part * per, (part + 1) * per):
                t = 8 * a + b
                wide[t] = sig[:, :, :, t * 128 : (t + 1) * 128].astype(F32).reshape(256, 128)

    def take_pulse(j, part, into, at):
        for b in range(part * per, (part + 1) * per):
            for a in range(4):
                into[at, b, a] = wide[8 * a + b, pl.ds(j, 32, stride=8), :].astype(BF16)

    def hop(k, part):
        t = lax.rem(me + HOPS[k] + NZ, NZ)
        mine = pl.ds(part * per, per)
        return t, pltpu.make_async_remote_copy(
            src_ref=send.at[t, mine], dst_ref=recv.at[me, mine], send_sem=ss1.at[k, part], recv_sem=rs1.at[k, part],
            device_id=zdev(t), device_id_type=MESH,
        )

    for part in range(CHUNKS):
        widen(part)
        for k in range(7):
            t, copy = hop(k, part)
            take_pulse(t, part, send, t)
            if k == 0 and part == 0:
                pl.semaphore_wait(bar, NZ - 1 + NQ - 1)
            copy.start()
    for part in range(CHUNKS):
        take_pulse(me, part, recv, me)

    for copy in fetched:
        copy.wait()
    wr, wi = steer[0].astype(F32), steer[1].astype(F32)
    wmat[0:32] = jnp.concatenate([wr, -wi], axis=1).astype(BF16)
    wmat[32:64] = jnp.concatenate([wi, wr], axis=1).astype(BF16)
    for i in range(2):
        for m in range(64):
            rowed[m : m + 1] = spec[i : i + 1, m * 128 : (m + 1) * 128]
        a = rowed[...] * (1.0 / 8192)
        both = jnp.concatenate([a, jnp.concatenate([a[:, 64:], a[:, :64]], axis=1)], axis=0)
        turned_resp[...] = jnp.transpose(both)
        for ka in range(8):
            resp[i, ka * 64 : ka * 64 + 64] = spread(turned_resp[pl.ds(ka, 8, stride=8), :])
            tw[i, ka * 64 : ka * 64 + 64] = spread(twist[i, ka * 8 : ka * 8 + 8])

    def front(b):
        now = b % 2
        for half in range(2):
            for a in (0, 2):
                blocks = []
                for e in range(2):
                    tiles = [recv[2 * cc + half, b, a + e] for cc in range(4)]
                    blocks.append(jnp.concatenate([t[:16] for t in tiles] + [t[16:] for t in tiles], axis=0))
                got = jnp.dot(wmat[...], jnp.concatenate(blocks, axis=1), preferred_element_type=F32)
                got = got.astype(BF16).astype(F32)
                for e in range(2):
                    formed[now, half * 4 + a + e] = got[:, e * 128 : (e + 1) * 128]
        for g in range(4):
            xs = [(formed[now, a, 8 * g : 8 * g + 8], formed[now, a, 32 + 8 * g : 40 + 8 * g]) for a in range(8)]
            ys = dft(xs, -1)
            for ka in range(8):
                mid[g, b * 8 + ka] = joined(times(ys[ka], b * ka, 64, -1))

    for part in range(CHUNKS):
        for k in range(7):
            hop(k, part)[1].wait_recv()
        for b in range(part * per, (part + 1) * per):
            front(b)

    def filter_group(g):
        for ka in range(8):
            here = slice(ka * 64, ka * 64 + 64)
            xs = dft([pair(mid[g, b * 8 + ka]) for b in range(8)], -1)
            tr, ti = tw[0, here], tw[1, here]
            re = jnp.concatenate([v[0] for v in xs], axis=0)
            im = jnp.concatenate([v[1] for v in xs], axis=0)
            lhs[here, 0:128] = (re * tr - im * ti).astype(BF16)
            lhs[here, 128:256] = (re * ti + im * tr).astype(BF16)
        prod[...] = jnp.dot(lhs[...], lanes[0], preferred_element_type=F32)
        for ka in range(8):
            here = slice(ka * 64, ka * 64 + 64)
            hr, hi = resp[0, here], resp[1, here]
            re, im = prod[here, 0:128], prod[here, 128:256]
            lhs[here, 0:128] = (re * hr - im * hi).astype(BF16)
            lhs[here, 128:256] = (re * hi + im * hr).astype(BF16)
        prod[...] = jnp.dot(lhs[...], lanes[1], preferred_element_type=F32)
        for ka in range(8):
            here = slice(ka * 64, ka * 64 + 64)
            tr, ti = tw[0, here], tw[1, here]
            re, im = prod[here, 0:128], prod[here, 128:256]
            re, im = re * tr + im * ti, im * tr - re * ti
            ys = dft([(re[8 * kb : 8 * kb + 8], im[8 * kb : 8 * kb + 8]) for kb in range(8)], 1)
            for b in range(8):
                mid2[b * 8 + ka] = joined(times(ys[b], b * ka, 64, 1))
        for b in range(8):
            xs = dft([pair(mid2[b * 8 + ka]) for ka in range(8)], 1)
            for a in range(8):
                n1 = 8 * a + b
                t = n1 if n1 < 32 else 63 - n1
                comp[g, 1 - t % 2, n1 // 32, t // 2] = joined(xs[a]).astype(BF16)

    k, i0 = 1 - lax.rem(q, 2), q // 2

    def chip(i, core):
        x, y = i0 // 4, lax.rem(i0, 4)
        return (lax.rem(x + i // 4, 4) * 4 + lax.rem(y + i % 4, 4)) * 2 + 1 - core

    def along(step, e, src, dst, ss, rs):
        g, rr = lax.rem(c + GROUPS[step], 4), lax.rem(r + e, 2)
        return pltpu.make_async_remote_copy(
            src_ref=src(g, rr), dst_ref=dst, send_sem=ss.at[step, e], recv_sem=rs.at[step, e],
            device_id={"chan": g, "range": rr}, device_id_type=MESH,
        )

    def first_set(step, e):
        return along(step, e, lambda g, rr: comp.at[g, 0, rr], early.at[me], ss3, rs3)

    def second_set(step, e):
        return along(step, e, lambda g, rr: crossed.at[g, rr], cols.at[me], ss7, rs7)

    def cross(g, i):
        t = chip(i, 1)
        return pltpu.make_async_remote_copy(
            src_ref=comp.at[g, 1, :, t // 2], dst_ref=crossed.at[g, :, q],
            send_sem=ss2.at[g, 0 if i else 1], recv_sem=rs2.at[g],
            device_id={"pulse": t}, device_id_type=MESH,
        )

    def forward(cs, i):
        t = chip(i, 0)
        pick = pl.ds(2 * cs, 2)
        return pltpu.make_async_remote_copy(
            src_ref=early.at[pick, t // 2], dst_ref=cols.at[pick, q], send_sem=ss6.at[0 if i else 1], recv_sem=rs6,
            device_id={"pulse": t}, device_id_type=MESH,
        )

    def send_group(step):
        g = lax.rem(c + GROUPS[step], 4)
        for e in range(2):
            if GROUPS[step] or e:
                first_set(step, e).start()
        for i in NEAR_LAST:
            cross(g, i).start()

        @pl.when(k == 0)
        def _():
            cross(g, 0).start()

        @pl.when(k == 1)
        def _():
            for rr in range(2):
                crossed[g, rr, q] = comp[g, 1, rr, i0]

    for step in range(4):
        filter_group(lax.rem(c + GROUPS[step], 4))
        send_group(step)
    for i in range(16):
        early[me, i] = comp[c, 0, r, i]

    def second_go(step):
        @pl.when(k == 1)
        def _():
            g = lax.rem(c + GROUPS[step], 4)
            whole = crossed.at[g, :, pl.ds(0, NQ - 1)]
            pltpu.make_async_copy(whole, whole, rs2.at[g]).wait()
            for e in range(2):
                if GROUPS[step] or e:
                    second_set(step, e).start()

    def first_go(step):
        cs = lax.rem(c - GROUPS[step] + 4, 4)
        for e in range(2):
            if GROUPS[step] or e:
                first_set(step, e).wait_recv()
        for i in NEAR_LAST:
            forward(cs, i).start()

        @pl.when(k == 1)
        def _():
            forward(cs, 0).start()

        @pl.when(k == 0)
        def _():
            for e in range(2):
                cols[2 * cs + e, q] = early[2 * cs + e, i0]

    second_go(0)
    second_go(1)
    first_go(0)
    second_go(2)
    first_go(1)
    second_go(3)
    first_go(2)
    first_go(3)

    @pl.when(k == 1)
    def _():
        def keep(t, carry):
            cols[me, t] = crossed[c, r, t]
            return carry

        lax.fori_loop(0, NQ, keep, 0, unroll=4)
        for step in range(4):
            for e in range(2):
                if GROUPS[step] or e:
                    second_set(step, e).wait_recv()

    @pl.when(k == 0)
    def _():
        whole = cols.at[:, pl.ds(0, NQ - 1)]
        pltpu.make_async_copy(whole, whole, rs6).wait()

    for b in range(16):
        ps = [16 * a + b for a in range(16)]
        ys = dft([pair(cols[p % 8, p // 8]) for p in ps], -1)
        for fa in range(16):
            dmid[b * 16 + fa] = joined(times(ys[fa], b * fa, 256, -1))
    def to_bins(core, i):
        t = lax.rem(i0 // 4 + i // 4, 4) * 8 + lax.rem(i0 + i, 4) * 2 + core
        return pltpu.make_async_remote_copy(
            src_ref=power.at[pl.ds(t * 8, 8)], dst_ref=rows.at[q], send_sem=ss4.at[core, i], recv_sem=rs4.at[q],
            device_id={"pulse": t}, device_id_type=MESH,
        )

    def from_bins(s):
        return pltpu.make_async_remote_copy(
            src_ref=power.at[pl.ds(s * 8, 8)], dst_ref=rows.at[s], send_sem=ss4.at[0, 0], recv_sem=rs4.at[s],
            device_id={"pulse": s}, device_id_type=MESH,
        )

    for core in range(2):
        for fa in range(core * 8, core * 8 + 8):
            xs = dft([pair(dmid[b * 16 + fa]) for b in range(16)], -1)
            for fb in range(16):
                re, im = xs[fb]
                power[fa + 16 * fb] = ((re * re + im * im) * (1.0 / 256)).astype(BF16)
        for i in NEAR_LAST:
            to_bins(core, i).start()

        @pl.when(lax.rem(q, 2) == 1 - core)
        def _():
            to_bins(core, 0).start()

    for part in range(CHUNKS):
        for h in range(7):
            hop(h, part)[1].wait_send()
    for step in range(4):
        for e in range(2):
            if GROUPS[step] or e:
                first_set(step, e).wait_send()
    for g in range(4):
        whole = comp.at[g, 1, :, pl.ds(0, 15)]
        pltpu.make_async_copy(whole, whole, ss2.at[g, 0]).wait()
    whole = early.at[:, pl.ds(0, 15)]
    pltpu.make_async_copy(whole, whole, ss6.at[0]).wait()

    @pl.when(k == 0)
    def _():
        for g in range(4):
            whole = comp.at[g, 1, :, 0]
            pltpu.make_async_copy(whole, whole, ss2.at[g, 1]).wait()

    @pl.when(k == 1)
    def _():
        whole = early.at[:, 0]
        pltpu.make_async_copy(whole, whole, ss6.at[1]).wait()
        for step in range(4):
            for e in range(2):
                if GROUPS[step] or e:
                    second_set(step, e).wait_send()

    rows[q] = power[pl.ds(q * 8, 8)]
    outer = NQ - 1

    def store(s):
        return pltpu.make_async_copy(rows.at[s], rows_hbm.at[s], stores)

    store(q).start()

    @pl.when(q != outer)
    def _():
        from_bins(outer).wait_recv()
        store(outer).start()

    edge = pltpu.make_async_remote_copy(
        src_ref=rows.at[outer], dst_ref=halo, send_sem=ss5, recv_sem=rs5,
        device_id={"range": 1 - r}, device_id_type=MESH,
    )
    edge.start()

    def wait_bins(d, carry):
        s = lax.rem(q + d, NQ)

        @pl.when(s != outer)
        def _():
            from_bins(s).wait_recv()
            store(s).start()

        return carry

    lax.fori_loop(1, NQ, wait_bins, 0)

    edge.wait()
    pltpu.make_async_copy(rows, rows_hbm, stores).wait()
    for core in range(2):
        for i in NEAR_LAST:
            to_bins(core, i).wait_send()

        @pl.when(lax.rem(q, 2) == 1 - core)
        def _():
            to_bins(core, 0).wait_send()


def band_table():
    gap = np.abs(np.arange(512)[:, None] - (128 + np.arange(256)[None, :]))
    return ((gap > GUARD) & (gap <= GUARD + TRAIN)).astype(np.float32)


def window(rows, halo, band, out_hbm, win, noise, turned, out, done):
    r = lax.axis_index("range")
    right = r.astype(F32)

    def tile(t):
        return rows[t + r * (31 - 2 * t)].astype(F32).reshape(64, 128)

    def place(i, at, x):
        win[i, :, at * 128 : (at + 1) * 128] = x

    beside = halo[...].astype(F32).reshape(64, 128)
    place(0, 0, (beside * right).astype(BF16))
    place(15, 3, (beside * (1.0 - right)).astype(BF16))
    for i in range(16):
        x0, x1 = tile(2 * i).astype(BF16), tile(2 * i + 1).astype(BF16)
        place(i, 1, x0)
        place(i, 2, x1)
        if i > 0:
            place(i - 1, 3, x0)
        if i < 15:
            place(i + 1, 0, x1)
    copies = []
    for part in range(4):
        here = slice(part * 4, part * 4 + 4)
        noise[part] = jnp.dot(win[here].reshape(256, 512), band[...], preferred_element_type=F32)
        for t in range(part * 8, part * 8 + 8):
            i, e = t // 2 - part * 4, t % 2
            level = noise[part, i * 64 : (i + 1) * 64, e * 128 : (e + 1) * 128]
            got = tile(t) / (level * (1.0 / (2 * TRAIN)) + NOISE_FLOOR)
            for f in range(8):
                turned[t, pl.ds(f, 8, stride=8), :] = got[f * 8 : f * 8 + 8]
            out[:, t * 128 : (t + 1) * 128] = turned[t]
        lanes = pl.ds(part * 1024, 1024)
        copies.append(pltpu.make_async_copy(out.at[:, lanes], out_hbm.at[:, lanes], done.at[part]))
        copies[-1].start()
    for copy in copies:
        copy.wait()


def shards(signal, steering, spectrum):
    lanes, twist = lane_tables()
    dma = pltpu.SemaphoreType.DMA
    hbm = pl.BlockSpec(memory_space=pl.ANY)
    scratch = [
        pltpu.VMEM((2, 16, 8, 4096), BF16),
        pltpu.VMEM((2, 32, 64), BF16),
        pltpu.VMEM((2, 8192), F32),
        pltpu.VMEM((2, 256, 256), BF16),
        pltpu.VMEM((2, 64, 128), F32),
        pltpu.VMEM((64, 128), BF16),
        pltpu.VMEM((64, 128), F32),
        pltpu.VMEM((128, 128), F32),
        pltpu.VMEM((2, 512, 128), F32),
        pltpu.VMEM((2, 512, 128), F32),
        pltpu.VMEM((32, 256, 128), F32),
        pltpu.VMEM((8, 8, 4, 32, 128), BF16),
        pltpu.VMEM((8, 8, 4, 32, 128), BF16),
        pltpu.VMEM((2, 8, 64, 128), F32),
        pltpu.VMEM((4, 64, 16, 128), F32),
        pltpu.VMEM((64, 16, 128), F32),
        pltpu.VMEM((512, 256), BF16),
        pltpu.VMEM((512, 256), F32),
        pltpu.VMEM((4, 2, 2, 16, 16, 128), BF16),
        pltpu.VMEM((4, 2, 32, 16, 128), BF16),
        pltpu.VMEM((8, 16, 16, 128), BF16),
        pltpu.VMEM((8, 32, 16, 128), BF16),
        pltpu.VMEM((256, 16, 128), F32),
        pltpu.VMEM((256, 8, 128), BF16),
        pltpu.VMEM((32, 8, 8, 128), BF16),
        dma((4,)), dma((CHUNKS, 4)),
        dma((7, CHUNKS)), dma((7, CHUNKS)),
        dma((4, 2)), dma((4,)),
        dma((4, 2)), dma((4, 2)),
        dma((2, 16)), dma((32,)),
        dma, dma,
        dma((2,)), dma,
        dma((4, 2)), dma((4, 2)),
        dma,
    ]
    rows, halo = pl.pallas_call(
        kernel,
        out_shape=[jax.ShapeDtypeStruct((32, 8, 8, 128), BF16), jax.ShapeDtypeStruct((8, 8, 128), BF16)],
        in_specs=[hbm] * 5,
        out_specs=[hbm, hbm],
        scratch_shapes=scratch,
        compiler_params=pltpu.CompilerParams(collective_id=0, has_side_effects=True, vmem_limit_bytes=60 * 2**20),
        name="radar",
    )(signal, steering, spectrum, jnp.asarray(lanes, BF16), jnp.asarray(twist, F32))
    got = pl.pallas_call(
        window,
        out_shape=jax.ShapeDtypeStruct((64, 4096), F32),
        in_specs=[pl.BlockSpec(memory_space=pltpu.VMEM)] * 3,
        out_specs=hbm,
        scratch_shapes=[
            pltpu.VMEM((16, 64, 512), BF16),
            pltpu.VMEM((4, 256, 256), F32),
            pltpu.VMEM((32, 64, 128), F32),
            pltpu.VMEM((64, 4096), F32),
            dma((4,)),
        ],
        compiler_params=pltpu.CompilerParams(vmem_limit_bytes=60 * 2**20),
        name="window",
    )(rows, halo, jnp.asarray(band_table(), BF16))
    return got.reshape(8, 8, 4096)


def solution(mesh):
    return jax.shard_map(
        shards,
        mesh=mesh,
        in_specs=(P(None, "chan", "pulse", "range"), P(), P()),
        out_specs=P("chan", "pulse", "range"),
        check_vma=False,
    )
```

```python
import math

import jax
import jax.numpy as jnp
import numpy as np
from jax import lax
from jax.experimental import pallas as pl
from jax.experimental.pallas import tpu as pltpu
from jax.sharding import PartitionSpec as P

F32, BF16 = jnp.float32, jnp.bfloat16
MESH = pl.DeviceIdType.MESH
GUARD, TRAIN, NOISE_FLOOR = 4, 16, 0.25
NZ, NQ = 8, 32
HOPS = (4, 3, -3, 2, -2, 1, -1)
GROUPS = (2, 1, 3, 0)
NEAR_LAST = (10, 6, 14, 9, 11, 5, 15, 7, 13, 8, 2, 4, 12, 1, 3)
CHUNKS = 8


def times(v, angle_num, period, sign):
    k = angle_num % period
    if k == 0:
        return v
    re, im = v
    if 4 * k == period:
        return (-im, re) if sign > 0 else (im, -re)
    if 2 * k == period:
        return (-re, -im)
    if 4 * k == 3 * period:
        return (im, -re) if sign > 0 else (-im, re)
    c = math.cos(2 * math.pi * k / period)
    s = sign * math.sin(2 * math.pi * k / period)
    return (re * c - im * s, re * s + im * c)


def dft(xs, sign):
    n = len(xs)
    if n == 1:
        return xs
    even, odd = dft(xs[0::2], sign), dft(xs[1::2], sign)
    odd = [times(v, k, n, sign) for k, v in enumerate(odd)]
    plus = [(a[0] + b[0], a[1] + b[1]) for a, b in zip(even, odd)]
    minus = [(a[0] - b[0], a[1] - b[1]) for a, b in zip(even, odd)]
    return plus + minus


def pair(x):
    x = x.astype(F32)
    return (x[:8], x[8:])


def joined(v):
    return jnp.concatenate(v, axis=0)


def lane_tables():
    n = np.arange(128)
    k2 = 2 * (n % 64) + n // 64
    ang = 2 * np.pi * (np.outer(n, k2) % 128) / 128
    c, s = np.cos(ang), np.sin(ang)
    ahead = np.block([[c, -s], [s, c]])
    back = np.block([[c.T, s.T], [-s.T, c.T]])
    k1 = (np.arange(8)[:, None] + 8 * np.arange(8)[None, :]).reshape(-1)
    turn = 2 * np.pi * np.outer(k1, n) / 8192
    twist = np.stack([np.cos(turn), -np.sin(turn)])
    return np.stack([ahead, back]), twist


def spread(rows):
    return jnp.broadcast_to(rows[:, None, :], (8, 8, 128)).reshape(64, 128)


def zdev(z):
    return {"chan": z // 2, "range": lax.rem(z, 2)}


def kernel(
    sig_hbm, steer_hbm, spec_hbm, lanes_hbm, twist_hbm, rows, halo,
    sig, steer, spec, lanes, twist, wmat, rowed, turned_resp, resp, tw,
    wide, send, recv, formed, mid, mid2, lhs, prod, comp, crossed, early, cols, dmid, power,
    loads, parts, ss1, rs1, ss2, rs2, ss3, rs3, ss4, rs4, ss5, rs5, ss6, rs6, ss7, rs7, stores,
):
    c, q, r = lax.axis_index("chan"), lax.axis_index("pulse"), lax.axis_index("range")
    me = c * 2 + r
    bar = pltpu.get_barrier_semaphore()
    for d in range(1, NZ):
        pl.semaphore_signal(bar, inc=1, device_id=zdev(lax.rem(me + d, NZ)), device_id_type=MESH)

    def greet(d, carry):
        pl.semaphore_signal(bar, inc=1, device_id={"pulse": lax.rem(q + d, NQ)}, device_id_type=MESH)
        return carry

    lax.fori_loop(1, NQ, greet, 0)
    fetched = [
        pltpu.make_async_copy(a, b, loads.at[i])
        for i, (a, b) in enumerate(
            [(steer_hbm, steer), (spec_hbm, spec), (lanes_hbm, lanes), (twist_hbm, twist)]
        )
    ]
    per = 8 // CHUNKS

    def drain(ref, sem):
        pltpu.make_async_copy(ref, ref, sem).wait()

    def part_copy(part, a):
        at = (slice(None), slice(None), slice(None), pl.ds((8 * a + part * per) * 128, per * 128))
        return pltpu.make_async_copy(sig_hbm.at[at], sig.at[at], parts.at[part])

    for part in range(CHUNKS):
        for a in range(4):
            part_copy(part, a).start()
    for copy in fetched:
        copy.start()

    def widen(part):
        drain(sig.at[:, :, :, pl.ds(0, 4 * per * 128)], parts.at[part])
        for a in range(4):
            for b in range(part * per, (part + 1) * per):
                t = 8 * a + b
                wide[t] = sig[:, :, :, t * 128 : (t + 1) * 128].astype(F32).reshape(256, 128)

    def take_pulse(j, part, into, at):
        for b in range(part * per, (part + 1) * per):
            for a in range(4):
                into[at, b, a] = wide[8 * a + b, pl.ds(j, 32, stride=8), :].astype(BF16)

    def hop(k, part):
        t = lax.rem(me + HOPS[k] + NZ, NZ)
        mine = pl.ds(part * per, per)
        return t, pltpu.make_async_remote_copy(
            src_ref=send.at[t, mine], dst_ref=recv.at[me, mine], send_sem=ss1, recv_sem=rs1.at[part],
            device_id=zdev(t), device_id_type=MESH,
        )

    for part in range(CHUNKS):
        widen(part)
        for k in range(7):
            t, copy = hop(k, part)
            take_pulse(t, part, send, t)
            if k == 0 and part == 0:
                pl.semaphore_wait(bar, NZ - 1 + NQ - 1)
            copy.start()
    for part in range(CHUNKS):
        take_pulse(me, part, recv, me)

    for copy in fetched:
        copy.wait()
    wr, wi = steer[0].astype(F32), steer[1].astype(F32)
    wmat[0:32] = jnp.concatenate([wr, -wi], axis=1).astype(BF16)
    wmat[32:64] = jnp.concatenate([wi, wr], axis=1).astype(BF16)
    for i in range(2):
        for m in range(64):
            rowed[m : m + 1] = spec[i : i + 1, m * 128 : (m + 1) * 128]
        a = rowed[...] * (1.0 / 8192)
        both = jnp.concatenate([a, jnp.concatenate([a[:, 64:], a[:, :64]], axis=1)], axis=0)
        turned_resp[...] = jnp.transpose(both)
        for ka in range(8):
            resp[i, ka * 64 : ka * 64 + 64] = spread(turned_resp[pl.ds(ka, 8, stride=8), :])
            tw[i, ka * 64 : ka * 64 + 64] = spread(twist[i, ka * 8 : ka * 8 + 8])

    def front(b):
        now = b % 2
        for half in range(2):
            for a in (0, 2):
                blocks = []
                for e in range(2):
                    tiles = [recv[2 * cc + half, b, a + e] for cc in range(4)]
                    blocks.append(jnp.concatenate([t[:16] for t in tiles] + [t[16:] for t in tiles], axis=0))
                got = jnp.dot(wmat[...], jnp.concatenate(blocks, axis=1), preferred_element_type=F32)
                got = got.astype(BF16).astype(F32)
                for e in range(2):
                    formed[now, half * 4 + a + e] = got[:, e * 128 : (e + 1) * 128]
        for g in range(4):
            xs = [(formed[now, a, 8 * g : 8 * g + 8], formed[now, a, 32 + 8 * g : 40 + 8 * g]) for a in range(8)]
            ys = dft(xs, -1)
            for ka in range(8):
                mid[g, b * 8 + ka] = joined(times(ys[ka], b * ka, 64, -1))

    for part in range(CHUNKS):
        drain(recv.at[pl.ds(0, 7), pl.ds(0, per)], rs1.at[part])
        for b in range(part * per, (part + 1) * per):
            front(b)

    def filter_group(g):
        for ka in range(8):
            here = slice(ka * 64, ka * 64 + 64)
            xs = dft([pair(mid[g, b * 8 + ka]) for b in range(8)], -1)
            tr, ti = tw[0, here], tw[1, here]
            re = jnp.concatenate([v[0] for v in xs], axis=0)
            im = jnp.concatenate([v[1] for v in xs], axis=0)
            lhs[here, 0:128] = (re * tr - im * ti).astype(BF16)
            lhs[here, 128:256] = (re * ti + im * tr).astype(BF16)
        prod[...] = jnp.dot(lhs[...], lanes[0], preferred_element_type=F32)
        for ka in range(8):
            here = slice(ka * 64, ka * 64 + 64)
            hr, hi = resp[0, here], resp[1, here]
            re, im = prod[here, 0:128], prod[here, 128:256]
            lhs[here, 0:128] = (re * hr - im * hi).astype(BF16)
            lhs[here, 128:256] = (re * hi + im * hr).astype(BF16)
        prod[...] = jnp.dot(lhs[...], lanes[1], preferred_element_type=F32)
        for ka in range(8):
            here = slice(ka * 64, ka * 64 + 64)
            tr, ti = tw[0, here], tw[1, here]
            re, im = prod[here, 0:128], prod[here, 128:256]
            re, im = re * tr + im * ti, im * tr - re * ti
            ys = dft([(re[8 * kb : 8 * kb + 8], im[8 * kb : 8 * kb + 8]) for kb in range(8)], 1)
            for b in range(8):
                mid2[b * 8 + ka] = joined(times(ys[b], b * ka, 64, 1))
        for b in range(8):
            xs = dft([pair(mid2[b * 8 + ka]) for ka in range(8)], 1)
            for a in range(8):
                n1 = 8 * a + b
                t = n1 if n1 < 32 else 63 - n1
                comp[g, 1 - t % 2, n1 // 32, t // 2] = joined(xs[a]).astype(BF16)

    k, i0 = 1 - lax.rem(q, 2), q // 2

    def chip(i, core):
        x, y = i0 // 4, lax.rem(i0, 4)
        return (lax.rem(x + i // 4, 4) * 4 + lax.rem(y + i % 4, 4)) * 2 + 1 - core

    def along(step, e, src, dst, ss, rs):
        g, rr = lax.rem(c + GROUPS[step], 4), lax.rem(r + e, 2)
        return pltpu.make_async_remote_copy(
            src_ref=src(g, rr), dst_ref=dst, send_sem=ss, recv_sem=rs,
            device_id={"chan": g, "range": rr}, device_id_type=MESH,
        )

    def first_set(step, e):
        return along(step, e, lambda g, rr: comp.at[g, 0, rr], early.at[me], ss3, rs3.at[step])

    def second_set(step, e):
        return along(step, e, lambda g, rr: crossed.at[g, rr], cols.at[me], ss7, rs7)

    def cross(g, i):
        t = chip(i, 1)
        return pltpu.make_async_remote_copy(
            src_ref=comp.at[g, 1, :, t // 2], dst_ref=crossed.at[g, :, q],
            send_sem=ss2, recv_sem=rs2.at[g],
            device_id={"pulse": t}, device_id_type=MESH,
        )

    def forward(cs, i):
        t = chip(i, 0)
        pick = pl.ds(2 * cs, 2)
        return pltpu.make_async_remote_copy(
            src_ref=early.at[pick, t // 2], dst_ref=cols.at[pick, q], send_sem=ss6, recv_sem=rs6,
            device_id={"pulse": t}, device_id_type=MESH,
        )

    def send_group(step):
        g = lax.rem(c + GROUPS[step], 4)
        for e in range(2):
            if GROUPS[step] or e:
                first_set(step, e).start()
        for i in NEAR_LAST:
            cross(g, i).start()

        @pl.when(k == 0)
        def _():
            cross(g, 0).start()

        @pl.when(k == 1)
        def _():
            for rr in range(2):
                crossed[g, rr, q] = comp[g, 1, rr, i0]

    for step in range(4):
        filter_group(lax.rem(c + GROUPS[step], 4))
        send_group(step)
    for i in range(16):
        early[me, i] = comp[c, 0, r, i]

    def second_go(step):
        @pl.when(k == 1)
        def _():
            g = lax.rem(c + GROUPS[step], 4)
            drain(crossed.at[g, :, pl.ds(0, NQ - 1)], rs2.at[g])
            for e in range(2):
                if GROUPS[step] or e:
                    second_set(step, e).start()

    def first_go(step):
        cs = lax.rem(c - GROUPS[step] + 4, 4)
        drain(early.at[pl.ds(0, 2 if GROUPS[step] else 1)], rs3.at[step])
        for i in NEAR_LAST:
            forward(cs, i).start()

        @pl.when(k == 1)
        def _():
            forward(cs, 0).start()

        @pl.when(k == 0)
        def _():
            for e in range(2):
                cols[2 * cs + e, q] = early[2 * cs + e, i0]

    second_go(0)
    second_go(1)
    first_go(0)
    second_go(2)
    first_go(1)
    second_go(3)
    first_go(2)
    first_go(3)

    @pl.when(k == 1)
    def _():
        def keep(t, carry):
            cols[me, t] = crossed[c, r, t]
            return carry

        lax.fori_loop(0, NQ, keep, 0, unroll=4)
        drain(cols.at[pl.ds(0, NZ - 1)], rs7)

    @pl.when(k == 0)
    def _():
        drain(cols.at[:, pl.ds(0, NQ - 1)], rs6)

    for b in range(16):
        ps = [16 * a + b for a in range(16)]
        ys = dft([pair(cols[p % 8, p // 8]) for p in ps], -1)
        for fa in range(16):
            dmid[b * 16 + fa] = joined(times(ys[fa], b * fa, 256, -1))
    def to_bins(core, i):
        t = lax.rem(i0 // 4 + i // 4, 4) * 8 + lax.rem(i0 + i, 4) * 2 + core
        return pltpu.make_async_remote_copy(
            src_ref=power.at[pl.ds(t * 8, 8)], dst_ref=rows.at[q], send_sem=ss4, recv_sem=rs4.at[q // (NQ - 1)],
            device_id={"pulse": t}, device_id_type=MESH,
        )

    for core in range(2):
        for fa in range(core * 8, core * 8 + 8):
            xs = dft([pair(dmid[b * 16 + fa]) for b in range(16)], -1)
            for fb in range(16):
                re, im = xs[fb]
                power[fa + 16 * fb] = ((re * re + im * im) * (1.0 / 256)).astype(BF16)
        for i in NEAR_LAST:
            to_bins(core, i).start()

        @pl.when(lax.rem(q, 2) == 1 - core)
        def _():
            to_bins(core, 0).start()

    drain(send.at[pl.ds(0, 7)], ss1)
    drain(early.at[pl.ds(0, NZ - 1)], ss3)

    @pl.when(k == 0)
    def _():
        drain(comp.at[:, 1], ss2)
        drain(early.at[:, pl.ds(0, 15)], ss6)

    @pl.when(k == 1)
    def _():
        drain(comp.at[:, 1, :, pl.ds(0, 15)], ss2)
        drain(early, ss6)
        drain(cols.at[pl.ds(0, NZ - 1)], ss7)

    own_rows = pltpu.make_async_copy(power.at[pl.ds(q * 8, 8)], rows.at[q], stores)
    own_rows.start()
    outer = NQ - 1

    @pl.when(q == outer)
    def _():
        own_rows.wait()

    @pl.when(q != outer)
    def _():
        drain(rows.at[outer], rs4.at[1])

    edge = pltpu.make_async_remote_copy(
        src_ref=rows.at[outer], dst_ref=halo, send_sem=ss5, recv_sem=rs5,
        device_id={"range": 1 - r}, device_id_type=MESH,
    )
    edge.start()

    @pl.when(q == outer)
    def _():
        drain(rows.at[pl.ds(0, NQ - 1)], rs4.at[0])

    @pl.when(q != outer)
    def _():
        drain(rows.at[pl.ds(0, NQ - 2)], rs4.at[0])
        own_rows.wait()

    edge.wait()
    drain(power.at[pl.ds(0, 8 * (NQ - 1))], ss4)


def band_table():
    gap = np.abs(np.arange(512)[:, None] - (128 + np.arange(256)[None, :]))
    return ((gap > GUARD) & (gap <= GUARD + TRAIN)).astype(np.float32)


def window(rows, halo, band, out_hbm, win, noise, turned, out, done):
    r = lax.axis_index("range")
    right = r.astype(F32)

    def tile(t):
        return rows[t + r * (31 - 2 * t)].astype(F32).reshape(64, 128)

    def place(i, at, x):
        win[i, :, at * 128 : (at + 1) * 128] = x

    beside = halo[...].astype(F32).reshape(64, 128)
    place(0, 0, (beside * right).astype(BF16))
    place(15, 3, (beside * (1.0 - right)).astype(BF16))
    for i in range(16):
        x0, x1 = tile(2 * i).astype(BF16), tile(2 * i + 1).astype(BF16)
        place(i, 1, x0)
        place(i, 2, x1)
        if i > 0:
            place(i - 1, 3, x0)
        if i < 15:
            place(i + 1, 0, x1)
    copies = []
    for part in range(4):
        here = slice(part * 4, part * 4 + 4)
        noise[part] = jnp.dot(win[here].reshape(256, 512), band[...], preferred_element_type=F32)
        for t in range(part * 8, part * 8 + 8):
            i, e = t // 2 - part * 4, t % 2
            level = noise[part, i * 64 : (i + 1) * 64, e * 128 : (e + 1) * 128]
            got = tile(t) / (level * (1.0 / (2 * TRAIN)) + NOISE_FLOOR)
            for f in range(8):
                turned[t, pl.ds(f, 8, stride=8), :] = got[f * 8 : f * 8 + 8]
            out[:, t * 128 : (t + 1) * 128] = turned[t]
        lanes = pl.ds(part * 1024, 1024)
        copies.append(pltpu.make_async_copy(out.at[:, lanes], out_hbm.at[:, lanes], done.at[part]))
        copies[-1].start()
    for copy in copies:
        copy.wait()


def shards(signal, steering, spectrum):
    lanes, twist = lane_tables()
    dma = pltpu.SemaphoreType.DMA
    hbm = pl.BlockSpec(memory_space=pl.ANY)
    scratch = [
        pltpu.VMEM((2, 16, 8, 4096), BF16),
        pltpu.VMEM((2, 32, 64), BF16),
        pltpu.VMEM((2, 8192), F32),
        pltpu.VMEM((2, 256, 256), BF16),
        pltpu.VMEM((2, 64, 128), F32),
        pltpu.VMEM((64, 128), BF16),
        pltpu.VMEM((64, 128), F32),
        pltpu.VMEM((128, 128), F32),
        pltpu.VMEM((2, 512, 128), F32),
        pltpu.VMEM((2, 512, 128), F32),
        pltpu.VMEM((32, 256, 128), F32),
        pltpu.VMEM((8, 8, 4, 32, 128), BF16),
        pltpu.VMEM((8, 8, 4, 32, 128), BF16),
        pltpu.VMEM((2, 8, 64, 128), F32),
        pltpu.VMEM((4, 64, 16, 128), F32),
        pltpu.VMEM((64, 16, 128), F32),
        pltpu.VMEM((512, 256), BF16),
        pltpu.VMEM((512, 256), F32),
        pltpu.VMEM((4, 2, 2, 16, 16, 128), BF16),
        pltpu.VMEM((4, 2, 32, 16, 128), BF16),
        pltpu.VMEM((8, 16, 16, 128), BF16),
        pltpu.VMEM((8, 32, 16, 128), BF16),
        pltpu.VMEM((256, 16, 128), F32),
        pltpu.VMEM((256, 8, 128), BF16),
        dma((4,)), dma((CHUNKS,)),
        dma, dma((CHUNKS,)),
        dma, dma((4,)),
        dma, dma((4,)),
        dma, dma((2,)),
        dma, dma,
        dma, dma,
        dma, dma,
        dma,
    ]
    rows, halo = pl.pallas_call(
        kernel,
        out_shape=[jax.ShapeDtypeStruct((32, 8, 8, 128), BF16), jax.ShapeDtypeStruct((8, 8, 128), BF16)],
        in_specs=[hbm] * 5,
        out_specs=[hbm, hbm],
        scratch_shapes=scratch,
        compiler_params=pltpu.CompilerParams(collective_id=0, has_side_effects=True, vmem_limit_bytes=60 * 2**20),
        name="radar",
    )(signal, steering, spectrum, jnp.asarray(lanes, BF16), jnp.asarray(twist, F32))
    got = pl.pallas_call(
        window,
        out_shape=jax.ShapeDtypeStruct((64, 4096), F32),
        in_specs=[pl.BlockSpec(memory_space=pltpu.VMEM)] * 3,
        out_specs=hbm,
        scratch_shapes=[
            pltpu.VMEM((16, 64, 512), BF16),
            pltpu.VMEM((4, 256, 256), F32),
            pltpu.VMEM((32, 64, 128), F32),
            pltpu.VMEM((64, 4096), F32),
            dma((4,)),
        ],
        compiler_params=pltpu.CompilerParams(vmem_limit_bytes=60 * 2**20),
        name="window",
    )(rows, halo, jnp.asarray(band_table(), BF16))
    return got.reshape(8, 8, 4096)


def solution(mesh):
    return jax.shard_map(
        shards,
        mesh=mesh,
        in_specs=(P(None, "chan", "pulse", "range"), P(), P()),
        out_specs=P("chan", "pulse", "range"),
        check_vma=False,
    )
```

```python
import math

import jax
import jax.numpy as jnp
import numpy as np
from jax import lax
from jax.experimental import pallas as pl
from jax.experimental.pallas import tpu as pltpu
from jax.sharding import PartitionSpec as P

F32, BF16 = jnp.float32, jnp.bfloat16
MESH = pl.DeviceIdType.MESH
GUARD, TRAIN, NOISE_FLOOR = 4, 16, 0.25
NZ, NQ = 8, 32
HOPS = (4, 3, -3, 2, -2, 1, -1)
GROUPS = (2, 1, 3, 0)
NEAR_LAST = (10, 6, 14, 9, 11, 5, 15, 7, 13, 8, 2, 4, 12, 1, 3)
CHUNKS = 8


def times(v, angle_num, period, sign):
    k = angle_num % period
    if k == 0:
        return v
    re, im = v
    if 4 * k == period:
        return (-im, re) if sign > 0 else (im, -re)
    if 2 * k == period:
        return (-re, -im)
    if 4 * k == 3 * period:
        return (im, -re) if sign > 0 else (-im, re)
    c = math.cos(2 * math.pi * k / period)
    s = sign * math.sin(2 * math.pi * k / period)
    return (re * c - im * s, re * s + im * c)


def dft(xs, sign):
    n = len(xs)
    if n == 1:
        return xs
    even, odd = dft(xs[0::2], sign), dft(xs[1::2], sign)
    odd = [times(v, k, n, sign) for k, v in enumerate(odd)]
    plus = [(a[0] + b[0], a[1] + b[1]) for a, b in zip(even, odd)]
    minus = [(a[0] - b[0], a[1] - b[1]) for a, b in zip(even, odd)]
    return plus + minus


def pair(x):
    x = x.astype(F32)
    return (x[:8], x[8:])


def joined(v):
    return jnp.concatenate(v, axis=0)


def lane_tables():
    n = np.arange(128)
    k2 = 2 * (n % 64) + n // 64
    ang = 2 * np.pi * (np.outer(n, k2) % 128) / 128
    c, s = np.cos(ang), np.sin(ang)
    ahead = np.block([[c, -s], [s, c]])
    back = np.block([[c.T, s.T], [-s.T, c.T]])
    k1 = (np.arange(8)[:, None] + 8 * np.arange(8)[None, :]).reshape(-1)
    turn = 2 * np.pi * np.outer(k1, n) / 8192
    twist = np.stack([np.cos(turn), -np.sin(turn)])
    return np.stack([ahead, back]), twist


def spread(rows):
    return jnp.broadcast_to(rows[:, None, :], (8, 8, 128)).reshape(64, 128)


def zdev(z):
    return {"chan": z // 2, "range": lax.rem(z, 2)}


def kernel(
    sig_hbm, steer_hbm, spec_hbm, lanes_hbm, twist_hbm, rows, halo,
    sig, steer, spec, lanes, twist, wmat, rowed, turned_resp, resp, tw,
    wide, send, recv, formed, mid, mid2, lhs, prod, comp, crossed, early, cols, dmid, power,
    loads, parts, ss1, rs1, ss2, rs2, ss3, rs3, ss4, rs4, ss5, rs5, ss6, rs6, ss7, rs7, stores,
):
    c, q, r = lax.axis_index("chan"), lax.axis_index("pulse"), lax.axis_index("range")
    me = c * 2 + r
    bar = pltpu.get_barrier_semaphore()
    for d in range(1, NZ):
        pl.semaphore_signal(bar, inc=1, device_id=zdev(lax.rem(me + d, NZ)), device_id_type=MESH)

    fetched = [
        pltpu.make_async_copy(a, b, loads.at[i])
        for i, (a, b) in enumerate(
            [(steer_hbm, steer), (spec_hbm, spec), (lanes_hbm, lanes), (twist_hbm, twist)]
        )
    ]
    per = 8 // CHUNKS

    def drain(ref, sem):
        pltpu.make_async_copy(ref, ref, sem).wait()

    def part_copy(part, a):
        at = (slice(None), slice(None), slice(None), pl.ds((8 * a + part * per) * 128, per * 128))
        return pltpu.make_async_copy(sig_hbm.at[at], sig.at[at], parts.at[part])

    for a in range(4):
        part_copy(0, a).start()

    def greet(d, carry):
        pl.semaphore_signal(bar, inc=1, device_id={"pulse": lax.rem(q + d, NQ)}, device_id_type=MESH)
        return carry

    lax.fori_loop(1, NQ, greet, 0, unroll=8)
    for part in range(1, CHUNKS):
        for a in range(4):
            part_copy(part, a).start()
    for copy in fetched:
        copy.start()

    def widen(part):
        drain(sig.at[:, :, :, pl.ds(0, 4 * per * 128)], parts.at[part])
        for a in range(4):
            for b in range(part * per, (part + 1) * per):
                t = 8 * a + b
                wide[t] = sig[:, :, :, t * 128 : (t + 1) * 128].astype(F32).reshape(256, 128)

    def take_pulse(j, part, into, at):
        for b in range(part * per, (part + 1) * per):
            for a in range(4):
                into[at, b, a] = wide[8 * a + b, pl.ds(j, 32, stride=8), :].astype(BF16)

    def hop(k, part):
        t = lax.rem(me + HOPS[k] + NZ, NZ)
        mine = pl.ds(part * per, per)
        return t, pltpu.make_async_remote_copy(
            src_ref=send.at[t, mine], dst_ref=recv.at[me, mine], send_sem=ss1, recv_sem=rs1.at[part],
            device_id=zdev(t), device_id_type=MESH,
        )

    for part in range(CHUNKS):
        widen(part)
        for k in range(7):
            t, copy = hop(k, part)
            take_pulse(t, part, send, t)
            if k == 0 and part == 0:
                pl.semaphore_wait(bar, NZ - 1 + NQ - 1)
            copy.start()
    for part in range(CHUNKS):
        take_pulse(me, part, recv, me)

    for copy in fetched:
        copy.wait()
    wr, wi = steer[0].astype(F32), steer[1].astype(F32)
    wmat[0:32] = jnp.concatenate([wr, -wi], axis=1).astype(BF16)
    wmat[32:64] = jnp.concatenate([wi, wr], axis=1).astype(BF16)
    for i in range(2):
        for m in range(64):
            rowed[m : m + 1] = spec[i : i + 1, m * 128 : (m + 1) * 128]
        a = rowed[...] * (1.0 / 8192)
        both = jnp.concatenate([a, jnp.concatenate([a[:, 64:], a[:, :64]], axis=1)], axis=0)
        turned_resp[...] = jnp.transpose(both)
        for ka in range(8):
            resp[i, ka * 64 : ka * 64 + 64] = spread(turned_resp[pl.ds(ka, 8, stride=8), :])
            tw[i, ka * 64 : ka * 64 + 64] = spread(twist[i, ka * 8 : ka * 8 + 8])

    def front(b):
        now = b % 2
        for half in range(2):
            for a in (0, 2):
                blocks = []
                for e in range(2):
                    tiles = [recv[2 * cc + half, b, a + e] for cc in range(4)]
                    blocks.append(jnp.concatenate([t[:16] for t in tiles] + [t[16:] for t in tiles], axis=0))
                got = jnp.dot(wmat[...], jnp.concatenate(blocks, axis=1), preferred_element_type=F32)
                got = got.astype(BF16).astype(F32)
                for e in range(2):
                    formed[now, half * 4 + a + e] = got[:, e * 128 : (e + 1) * 128]
        for g in range(4):
            xs = [(formed[now, a, 8 * g : 8 * g + 8], formed[now, a, 32 + 8 * g : 40 + 8 * g]) for a in range(8)]
            ys = dft(xs, -1)
            for ka in range(8):
                mid[g, b * 8 + ka] = joined(times(ys[ka], b * ka, 64, -1))

    for part in range(CHUNKS):
        drain(recv.at[pl.ds(0, 7), pl.ds(0, per)], rs1.at[part])
        for b in range(part * per, (part + 1) * per):
            front(b)

    def filter_group(g):
        for ka in range(8):
            here = slice(ka * 64, ka * 64 + 64)
            xs = dft([pair(mid[g, b * 8 + ka]) for b in range(8)], -1)
            tr, ti = tw[0, here], tw[1, here]
            re = jnp.concatenate([v[0] for v in xs], axis=0)
            im = jnp.concatenate([v[1] for v in xs], axis=0)
            lhs[here, 0:128] = (re * tr - im * ti).astype(BF16)
            lhs[here, 128:256] = (re * ti + im * tr).astype(BF16)
        prod[...] = jnp.dot(lhs[...], lanes[0], preferred_element_type=F32)
        for ka in range(8):
            here = slice(ka * 64, ka * 64 + 64)
            hr, hi = resp[0, here], resp[1, here]
            re, im = prod[here, 0:128], prod[here, 128:256]
            lhs[here, 0:128] = (re * hr - im * hi).astype(BF16)
            lhs[here, 128:256] = (re * hi + im * hr).astype(BF16)
        prod[...] = jnp.dot(lhs[...], lanes[1], preferred_element_type=F32)
        for ka in range(8):
            here = slice(ka * 64, ka * 64 + 64)
            tr, ti = tw[0, here], tw[1, here]
            re, im = prod[here, 0:128], prod[here, 128:256]
            re, im = re * tr + im * ti, im * tr - re * ti
            ys = dft([(re[8 * kb : 8 * kb + 8], im[8 * kb : 8 * kb + 8]) for kb in range(8)], 1)
            for b in range(8):
                mid2[b * 8 + ka] = joined(times(ys[b], b * ka, 64, 1))
        for b in range(8):
            xs = dft([pair(mid2[b * 8 + ka]) for ka in range(8)], 1)
            for a in range(8):
                n1 = 8 * a + b
                t = n1 if n1 < 32 else 63 - n1
                comp[g, 1 - t % 2, n1 // 32, t // 2] = joined(xs[a]).astype(BF16)

    k, i0 = 1 - lax.rem(q, 2), q // 2

    def chip(i, core):
        x, y = i0 // 4, lax.rem(i0, 4)
        return (lax.rem(x + i // 4, 4) * 4 + lax.rem(y + i % 4, 4)) * 2 + 1 - core

    def along(step, e, src, dst, ss, rs):
        g, rr = lax.rem(c + GROUPS[step], 4), lax.rem(r + e, 2)
        return pltpu.make_async_remote_copy(
            src_ref=src(g, rr), dst_ref=dst, send_sem=ss, recv_sem=rs,
            device_id={"chan": g, "range": rr}, device_id_type=MESH,
        )

    def first_set(step, e):
        return along(step, e, lambda g, rr: comp.at[g, 0, rr], early.at[me], ss3, rs3.at[step])

    def second_set(step, e):
        return along(step, e, lambda g, rr: crossed.at[g, rr], cols.at[me], ss7, rs7)

    def cross(g, i):
        t = chip(i, 1)
        return pltpu.make_async_remote_copy(
            src_ref=comp.at[g, 1, :, t // 2], dst_ref=crossed.at[g, :, q],
            send_sem=ss2, recv_sem=rs2.at[g],
            device_id={"pulse": t}, device_id_type=MESH,
        )

    def forward(cs, i):
        t = chip(i, 0)
        pick = pl.ds(2 * cs, 2)
        return pltpu.make_async_remote_copy(
            src_ref=early.at[pick, t // 2], dst_ref=cols.at[pick, q], send_sem=ss6, recv_sem=rs6,
            device_id={"pulse": t}, device_id_type=MESH,
        )

    def send_group(step):
        g = lax.rem(c + GROUPS[step], 4)
        for e in range(2):
            if GROUPS[step] or e:
                first_set(step, e).start()
        for i in NEAR_LAST:
            cross(g, i).start()

        @pl.when(k == 0)
        def _():
            cross(g, 0).start()

        @pl.when(k == 1)
        def _():
            for rr in range(2):
                crossed[g, rr, q] = comp[g, 1, rr, i0]

    for step in range(4):
        filter_group(lax.rem(c + GROUPS[step], 4))
        send_group(step)
    for i in range(16):
        early[me, i] = comp[c, 0, r, i]

    def second_go(step):
        @pl.when(k == 1)
        def _():
            g = lax.rem(c + GROUPS[step], 4)
            drain(crossed.at[g, :, pl.ds(0, NQ - 1)], rs2.at[g])
            for e in range(2):
                if GROUPS[step] or e:
                    second_set(step, e).start()

    def first_go(step):
        cs = lax.rem(c - GROUPS[step] + 4, 4)
        drain(early.at[pl.ds(0, 2 if GROUPS[step] else 1)], rs3.at[step])
        for i in NEAR_LAST:
            forward(cs, i).start()

        @pl.when(k == 1)
        def _():
            forward(cs, 0).start()

        @pl.when(k == 0)
        def _():
            for e in range(2):
                cols[2 * cs + e, q] = early[2 * cs + e, i0]

    second_go(0)
    second_go(1)
    first_go(0)
    second_go(2)
    first_go(1)
    second_go(3)
    first_go(2)
    first_go(3)

    @pl.when(k == 1)
    def _():
        def keep(t, carry):
            cols[me, t] = crossed[c, r, t]
            return carry

        lax.fori_loop(0, NQ, keep, 0, unroll=4)
        drain(cols.at[pl.ds(0, NZ - 1)], rs7)

    @pl.when(k == 0)
    def _():
        drain(cols.at[:, pl.ds(0, NQ - 1)], rs6)

    for b in range(16):
        ps = [16 * a + b for a in range(16)]
        ys = dft([pair(cols[p % 8, p // 8]) for p in ps], -1)
        for fa in range(16):
            dmid[b * 16 + fa] = joined(times(ys[fa], b * fa, 256, -1))
    def to_bins(core, i):
        t = lax.rem(i0 // 4 + i // 4, 4) * 8 + lax.rem(i0 + i, 4) * 2 + core
        return pltpu.make_async_remote_copy(
            src_ref=power.at[pl.ds(t * 8, 8)], dst_ref=rows.at[q], send_sem=ss4, recv_sem=rs4.at[q // (NQ - 1)],
            device_id={"pulse": t}, device_id_type=MESH,
        )

    for core in range(2):
        for fa in range(core * 8, core * 8 + 8):
            xs = dft([pair(dmid[b * 16 + fa]) for b in range(16)], -1)
            for fb in range(16):
                re, im = xs[fb]
                power[fa + 16 * fb] = ((re * re + im * im) * (1.0 / 256)).astype(BF16)
        for i in NEAR_LAST:
            to_bins(core, i).start()

        @pl.when(lax.rem(q, 2) == 1 - core)
        def _():
            to_bins(core, 0).start()

    drain(send.at[pl.ds(0, 7)], ss1)
    drain(early.at[pl.ds(0, NZ - 1)], ss3)

    @pl.when(k == 0)
    def _():
        drain(comp.at[:, 1], ss2)
        drain(early.at[:, pl.ds(0, 15)], ss6)

    @pl.when(k == 1)
    def _():
        drain(comp.at[:, 1, :, pl.ds(0, 15)], ss2)
        drain(early, ss6)
        drain(cols.at[pl.ds(0, NZ - 1)], ss7)

    own_rows = pltpu.make_async_copy(power.at[pl.ds(q * 8, 8)], rows.at[q], stores)
    own_rows.start()
    outer = NQ - 1

    @pl.when(q == outer)
    def _():
        own_rows.wait()

    @pl.when(q != outer)
    def _():
        drain(rows.at[outer], rs4.at[1])

    edge = pltpu.make_async_remote_copy(
        src_ref=rows.at[outer], dst_ref=halo, send_sem=ss5, recv_sem=rs5,
        device_id={"range": 1 - r}, device_id_type=MESH,
    )
    edge.start()

    @pl.when(q == outer)
    def _():
        drain(rows.at[pl.ds(0, NQ - 1)], rs4.at[0])

    @pl.when(q != outer)
    def _():
        drain(rows.at[pl.ds(0, NQ - 2)], rs4.at[0])
        own_rows.wait()

    edge.wait()
    drain(power.at[pl.ds(0, 8 * (NQ - 1))], ss4)


def band_table():
    gap = np.abs(np.arange(512)[:, None] - (128 + np.arange(256)[None, :]))
    return ((gap > GUARD) & (gap <= GUARD + TRAIN)).astype(np.float32)


def window(rows, halo, band, out_hbm, win, noise, turned, out, done):
    r = lax.axis_index("range")
    right = r.astype(F32)

    def tile(t):
        return rows[t + r * (31 - 2 * t)].astype(F32).reshape(64, 128)

    def place(i, at, x):
        win[i, :, at * 128 : (at + 1) * 128] = x

    beside = halo[...].astype(F32).reshape(64, 128)
    place(0, 0, (beside * right).astype(BF16))
    place(15, 3, (beside * (1.0 - right)).astype(BF16))
    for i in range(16):
        x0, x1 = tile(2 * i).astype(BF16), tile(2 * i + 1).astype(BF16)
        place(i, 1, x0)
        place(i, 2, x1)
        if i > 0:
            place(i - 1, 3, x0)
        if i < 15:
            place(i + 1, 0, x1)
    copies = []
    for part in range(4):
        here = slice(part * 4, part * 4 + 4)
        noise[part] = jnp.dot(win[here].reshape(256, 512), band[...], preferred_element_type=F32)
        for t in range(part * 8, part * 8 + 8):
            i, e = t // 2 - part * 4, t % 2
            level = noise[part, i * 64 : (i + 1) * 64, e * 128 : (e + 1) * 128]
            got = tile(t) / (level * (1.0 / (2 * TRAIN)) + NOISE_FLOOR)
            for f in range(8):
                turned[t, pl.ds(f, 8, stride=8), :] = got[f * 8 : f * 8 + 8]
            out[:, t * 128 : (t + 1) * 128] = turned[t]
        lanes = pl.ds(part * 1024, 1024)
        copies.append(pltpu.make_async_copy(out.at[:, lanes], out_hbm.at[:, lanes], done.at[part]))
        copies[-1].start()
    for copy in copies:
        copy.wait()


def shards(signal, steering, spectrum):
    lanes, twist = lane_tables()
    dma = pltpu.SemaphoreType.DMA
    hbm = pl.BlockSpec(memory_space=pl.ANY)
    scratch = [
        pltpu.VMEM((2, 16, 8, 4096), BF16),
        pltpu.VMEM((2, 32, 64), BF16),
        pltpu.VMEM((2, 8192), F32),
        pltpu.VMEM((2, 256, 256), BF16),
        pltpu.VMEM((2, 64, 128), F32),
        pltpu.VMEM((64, 128), BF16),
        pltpu.VMEM((64, 128), F32),
        pltpu.VMEM((128, 128), F32),
        pltpu.VMEM((2, 512, 128), F32),
        pltpu.VMEM((2, 512, 128), F32),
        pltpu.VMEM((32, 256, 128), F32),
        pltpu.VMEM((8, 8, 4, 32, 128), BF16),
        pltpu.VMEM((8, 8, 4, 32, 128), BF16),
        pltpu.VMEM((2, 8, 64, 128), F32),
        pltpu.VMEM((4, 64, 16, 128), F32),
        pltpu.VMEM((64, 16, 128), F32),
        pltpu.VMEM((512, 256), BF16),
        pltpu.VMEM((512, 256), F32),
        pltpu.VMEM((4, 2, 2, 16, 16, 128), BF16),
        pltpu.VMEM((4, 2, 32, 16, 128), BF16),
        pltpu.VMEM((8, 16, 16, 128), BF16),
        pltpu.VMEM((8, 32, 16, 128), BF16),
        pltpu.VMEM((256, 16, 128), F32),
        pltpu.VMEM((256, 8, 128), BF16),
        dma((4,)), dma((CHUNKS,)),
        dma, dma((CHUNKS,)),
        dma, dma((4,)),
        dma, dma((4,)),
        dma, dma((2,)),
        dma, dma,
        dma, dma,
        dma, dma,
        dma,
    ]
    rows, halo = pl.pallas_call(
        kernel,
        out_shape=[jax.ShapeDtypeStruct((32, 8, 8, 128), BF16), jax.ShapeDtypeStruct((8, 8, 128), BF16)],
        in_specs=[hbm] * 5,
        out_specs=[hbm, hbm],
        scratch_shapes=scratch,
        compiler_params=pltpu.CompilerParams(collective_id=0, has_side_effects=True, vmem_limit_bytes=60 * 2**20),
        name="radar",
    )(signal, steering, spectrum, jnp.asarray(lanes, BF16), jnp.asarray(twist, F32))
    got = pl.pallas_call(
        window,
        out_shape=jax.ShapeDtypeStruct((64, 4096), F32),
        in_specs=[pl.BlockSpec(memory_space=pltpu.VMEM)] * 3,
        out_specs=hbm,
        scratch_shapes=[
            pltpu.VMEM((16, 64, 512), BF16),
            pltpu.VMEM((4, 256, 256), F32),
            pltpu.VMEM((32, 64, 128), F32),
            pltpu.VMEM((64, 4096), F32),
            dma((4,)),
        ],
        compiler_params=pltpu.CompilerParams(vmem_limit_bytes=60 * 2**20),
        name="window",
    )(rows, halo, jnp.asarray(band_table(), BF16))
    return got.reshape(8, 8, 4096)


def solution(mesh):
    return jax.shard_map(
        shards,
        mesh=mesh,
        in_specs=(P(None, "chan", "pulse", "range"), P(), P()),
        out_specs=P("chan", "pulse", "range"),
        check_vma=False,
    )
```

```python
import math

import jax
import jax.numpy as jnp
import numpy as np
from jax import lax
from jax.experimental import pallas as pl
from jax.experimental.pallas import tpu as pltpu
from jax.sharding import PartitionSpec as P

F32, BF16 = jnp.float32, jnp.bfloat16
MESH = pl.DeviceIdType.MESH
GUARD, TRAIN, NOISE_FLOOR = 4, 16, 0.25
NZ, NQ = 8, 32
HOPS = (4, 3, -3, 2, -2, 1, -1)
GROUPS = (2, 1, 3, 0)
NEAR_LAST = (10, 6, 14, 9, 11, 5, 15, 7, 13, 8, 2, 4, 12, 1, 3)
CHUNKS = 8


def times(v, angle_num, period, sign):
    k = angle_num % period
    if k == 0:
        return v
    re, im = v
    if 4 * k == period:
        return (-im, re) if sign > 0 else (im, -re)
    if 2 * k == period:
        return (-re, -im)
    if 4 * k == 3 * period:
        return (im, -re) if sign > 0 else (-im, re)
    c = math.cos(2 * math.pi * k / period)
    s = sign * math.sin(2 * math.pi * k / period)
    return (re * c - im * s, re * s + im * c)


def dft(xs, sign):
    n = len(xs)
    if n == 1:
        return xs
    even, odd = dft(xs[0::2], sign), dft(xs[1::2], sign)
    odd = [times(v, k, n, sign) for k, v in enumerate(odd)]
    plus = [(a[0] + b[0], a[1] + b[1]) for a, b in zip(even, odd)]
    minus = [(a[0] - b[0], a[1] - b[1]) for a, b in zip(even, odd)]
    return plus + minus


def pair(x):
    x = x.astype(F32)
    return (x[:8], x[8:])


def joined(v):
    return jnp.concatenate(v, axis=0)


def lane_tables():
    n = np.arange(128)
    k2 = 2 * (n % 64) + n // 64
    ang = 2 * np.pi * (np.outer(n, k2) % 128) / 128
    c, s = np.cos(ang), np.sin(ang)
    ahead = np.block([[c, -s], [s, c]])
    back = np.block([[c.T, s.T], [-s.T, c.T]])
    k1 = (np.arange(8)[:, None] + 8 * np.arange(8)[None, :]).reshape(-1)
    turn = 2 * np.pi * np.outer(k1, n) / 8192
    twist = np.stack([np.cos(turn), -np.sin(turn)])
    return np.stack([ahead, back]), twist


def spread(rows):
    return jnp.broadcast_to(rows[:, None, :], (8, 8, 128)).reshape(64, 128)


def zdev(z):
    return {"chan": z // 2, "range": lax.rem(z, 2)}


def kernel(
    sig_hbm, steer_hbm, spec_hbm, lanes_hbm, twist_hbm, rows, halo,
    sig, steer, spec, lanes, twist, wmat, rowed, turned_resp, resp, tw,
    wide, send, recv, formed, mid, mid2, lhs, prod, comp, crossed, early, cols, dmid, power,
    loads, parts, ss1, rs1, ss2, rs2, ss3, rs3, ss4, rs4, ss5, rs5, ss6, rs6, ss7, rs7, stores,
):
    c, q, r = lax.axis_index("chan"), lax.axis_index("pulse"), lax.axis_index("range")
    me = c * 2 + r
    bar = pltpu.get_barrier_semaphore()
    for d in range(1, NZ):
        pl.semaphore_signal(bar, inc=1, device_id=zdev(lax.rem(me + d, NZ)), device_id_type=MESH)

    fetched = [
        pltpu.make_async_copy(a, b, loads.at[i])
        for i, (a, b) in enumerate(
            [(steer_hbm, steer), (spec_hbm, spec), (lanes_hbm, lanes), (twist_hbm, twist)]
        )
    ]
    per = 8 // CHUNKS

    def drain(ref, sem):
        pltpu.make_async_copy(ref, ref, sem).wait()

    def part_copy(part, a):
        at = (slice(None), slice(None), slice(None), pl.ds((8 * a + part * per) * 128, per * 128))
        return pltpu.make_async_copy(sig_hbm.at[at], sig.at[at], parts.at[part])

    for a in range(4):
        part_copy(0, a).start()

    def greet(d, carry):
        pl.semaphore_signal(bar, inc=1, device_id={"pulse": lax.rem(q + d, NQ)}, device_id_type=MESH)
        return carry

    lax.fori_loop(1, NQ, greet, 0, unroll=8)
    for part in range(1, CHUNKS):
        for a in range(4):
            part_copy(part, a).start()
    for copy in fetched:
        copy.start()

    def widen(part):
        drain(sig.at[:, :, :, pl.ds(0, 4 * per * 128)], parts.at[part])
        for a in range(4):
            for b in range(part * per, (part + 1) * per):
                t = 8 * a + b
                wide[t] = sig[:, :, :, t * 128 : (t + 1) * 128].astype(F32).reshape(256, 128)

    def take_pulse(j, part, into, at):
        for b in range(part * per, (part + 1) * per):
            for a in range(4):
                into[at, b, a] = wide[8 * a + b, pl.ds(j, 32, stride=8), :].astype(BF16)

    def hop(k, part):
        t = lax.rem(me + HOPS[k] + NZ, NZ)
        mine = pl.ds(part * per, per)
        return t, pltpu.make_async_remote_copy(
            src_ref=send.at[t, mine], dst_ref=recv.at[me, mine], send_sem=ss1, recv_sem=rs1.at[part],
            device_id=zdev(t), device_id_type=MESH,
        )

    for part in range(CHUNKS):
        widen(part)
        for k in range(7):
            t, copy = hop(k, part)
            take_pulse(t, part, send, t)
            if k == 0 and part == 0:
                pl.semaphore_wait(bar, NZ - 1 + NQ - 1)
            copy.start()
    for part in range(CHUNKS):
        take_pulse(me, part, recv, me)

    for copy in fetched:
        copy.wait()
    wr, wi = steer[0].astype(F32), steer[1].astype(F32)
    wmat[0:32] = jnp.concatenate([wr, -wi], axis=1).astype(BF16)
    wmat[32:64] = jnp.concatenate([wi, wr], axis=1).astype(BF16)
    for i in range(2):
        for m in range(64):
            rowed[m : m + 1] = spec[i : i + 1, m * 128 : (m + 1) * 128]
        a = rowed[...] * (1.0 / 8192)
        both = jnp.concatenate([a, jnp.concatenate([a[:, 64:], a[:, :64]], axis=1)], axis=0)
        turned_resp[...] = jnp.transpose(both)
        for ka in range(8):
            resp[i, ka * 64 : ka * 64 + 64] = spread(turned_resp[pl.ds(ka, 8, stride=8), :])
            tw[i, ka * 64 : ka * 64 + 64] = spread(twist[i, ka * 8 : ka * 8 + 8])

    def front(b):
        now = b % 2
        for half in range(2):
            for a in (0, 2):
                blocks = []
                for e in range(2):
                    tiles = [recv[2 * cc + half, b, a + e] for cc in range(4)]
                    blocks.append(jnp.concatenate([t[:16] for t in tiles] + [t[16:] for t in tiles], axis=0))
                got = jnp.dot(wmat[...], jnp.concatenate(blocks, axis=1), preferred_element_type=F32)
                got = got.astype(BF16).astype(F32)
                for e in range(2):
                    formed[now, half * 4 + a + e] = got[:, e * 128 : (e + 1) * 128]
        for g in range(4):
            xs = [(formed[now, a, 8 * g : 8 * g + 8], formed[now, a, 32 + 8 * g : 40 + 8 * g]) for a in range(8)]
            ys = dft(xs, -1)
            for ka in range(8):
                mid[g, b * 8 + ka] = joined(times(ys[ka], b * ka, 64, -1))

    for part in range(CHUNKS):
        drain(recv.at[pl.ds(0, 7), pl.ds(0, per)], rs1.at[part])
        for b in range(part * per, (part + 1) * per):
            front(b)

    def filter_group(g):
        for ka in range(8):
            here = slice(ka * 64, ka * 64 + 64)
            xs = dft([pair(mid[g, b * 8 + ka]) for b in range(8)], -1)
            tr, ti = tw[0, here], tw[1, here]
            re = jnp.concatenate([v[0] for v in xs], axis=0)
            im = jnp.concatenate([v[1] for v in xs], axis=0)
            lhs[here, 0:128] = (re * tr - im * ti).astype(BF16)
            lhs[here, 128:256] = (re * ti + im * tr).astype(BF16)
        prod[...] = jnp.dot(lhs[...], lanes[0], preferred_element_type=F32)
        for ka in range(8):
            here = slice(ka * 64, ka * 64 + 64)
            hr, hi = resp[0, here], resp[1, here]
            re, im = prod[here, 0:128], prod[here, 128:256]
            lhs[here, 0:128] = (re * hr - im * hi).astype(BF16)
            lhs[here, 128:256] = (re * hi + im * hr).astype(BF16)
        prod[...] = jnp.dot(lhs[...], lanes[1], preferred_element_type=F32)
        for ka in range(8):
            here = slice(ka * 64, ka * 64 + 64)
            tr, ti = tw[0, here], tw[1, here]
            re, im = prod[here, 0:128], prod[here, 128:256]
            re, im = re * tr + im * ti, im * tr - re * ti
            ys = dft([(re[8 * kb : 8 * kb + 8], im[8 * kb : 8 * kb + 8]) for kb in range(8)], 1)
            for b in range(8):
                mid2[b * 8 + ka] = joined(times(ys[b], b * ka, 64, 1))
        for b in range(8):
            xs = dft([pair(mid2[b * 8 + ka]) for ka in range(8)], 1)
            for a in range(8):
                n1 = 8 * a + b
                t = n1 if n1 < 32 else 63 - n1
                comp[g, 1 - t % 2, n1 // 32, t // 2] = joined(xs[a]).astype(BF16)

    k, i0 = 1 - lax.rem(q, 2), q // 2

    def chip(i, core):
        x, y = i0 // 4, lax.rem(i0, 4)
        return (lax.rem(x + i // 4, 4) * 4 + lax.rem(y + i % 4, 4)) * 2 + 1 - core

    def along(step, e, src, dst, ss, rs):
        g, rr = lax.rem(c + GROUPS[step], 4), lax.rem(r + e, 2)
        return pltpu.make_async_remote_copy(
            src_ref=src(g, rr), dst_ref=dst, send_sem=ss, recv_sem=rs,
            device_id={"chan": g, "range": rr}, device_id_type=MESH,
        )

    def slot(step):
        return 2 * ((1 - GROUPS[step]) % 4)

    def first_set(step, e):
        return along(step, e, lambda g, rr: comp.at[g, 0, rr], early.at[slot(step) + r], ss3, rs3.at[step])

    def second_set(step, e):
        return along(step, e, lambda g, rr: crossed.at[g, rr], cols.at[slot(step) + r], ss7, rs7)

    def cross(g, i):
        t = chip(i, 1)
        return pltpu.make_async_remote_copy(
            src_ref=comp.at[g, 1, :, t // 2], dst_ref=crossed.at[g, :, q],
            send_sem=ss2, recv_sem=rs2.at[g],
            device_id={"pulse": t}, device_id_type=MESH,
        )

    def forward(at, count, i):
        t = chip(i, 0)
        return pltpu.make_async_remote_copy(
            src_ref=early.at[pl.ds(at, count), t // 2], dst_ref=cols.at[pl.ds(at, count), q], send_sem=ss6, recv_sem=rs6,
            device_id={"pulse": t}, device_id_type=MESH,
        )

    def send_group(step):
        g = lax.rem(c + GROUPS[step], 4)
        for e in range(2):
            if GROUPS[step] or e:
                first_set(step, e).start()
        for i in NEAR_LAST:
            cross(g, i).start()

        @pl.when(k == 0)
        def _():
            cross(g, 0).start()

        @pl.when(k == 1)
        def _():
            for rr in range(2):
                crossed[g, rr, q] = comp[g, 1, rr, i0]

    for step in range(4):
        filter_group(lax.rem(c + GROUPS[step], 4))
        send_group(step)
    for i in range(16):
        early[slot(3) + r, i] = comp[c, 0, r, i]

    def second_go(step):
        @pl.when(k == 1)
        def _():
            g = lax.rem(c + GROUPS[step], 4)
            drain(crossed.at[g, :, pl.ds(0, NQ - 1)], rs2.at[g])
            for e in range(2):
                if GROUPS[step] or e:
                    second_set(step, e).start()

    def first_go(steps, at, count):
        for step in steps:
            drain(early.at[pl.ds(0, 2 if GROUPS[step] else 1)], rs3.at[step])
        for i in NEAR_LAST:
            forward(at, count, i).start()

        @pl.when(k == 1)
        def _():
            forward(at, count, 0).start()

        @pl.when(k == 0)
        def _():
            for z in range(at, at + count):
                cols[z, q] = early[z, i0]

    second_go(0)
    second_go(1)
    first_go((0,), 6, 2)
    second_go(2)
    second_go(3)
    first_go((1, 2, 3), 0, 6)

    @pl.when(k == 1)
    def _():
        def keep(t, carry):
            cols[slot(3) + r, t] = crossed[c, r, t]
            return carry

        lax.fori_loop(0, NQ, keep, 0, unroll=4)
        drain(cols.at[pl.ds(0, NZ - 1)], rs7)

    @pl.when(k == 0)
    def _():
        drain(cols.at[:, pl.ds(0, NQ - 1)], rs6)

    places = [2 * lax.rem(cs - c + 5, 4) for cs in range(4)]
    for b in range(16):
        ps = [16 * a + b for a in range(16)]
        ys = dft([pair(cols[places[p % 8 // 2] + p % 2, p // 8]) for p in ps], -1)
        for fa in range(16):
            dmid[b * 16 + fa] = joined(times(ys[fa], b * fa, 256, -1))
    def to_bins(core, i):
        t = lax.rem(i0 // 4 + i // 4, 4) * 8 + lax.rem(i0 + i, 4) * 2 + core
        return pltpu.make_async_remote_copy(
            src_ref=power.at[pl.ds(t * 8, 8)], dst_ref=rows.at[q], send_sem=ss4, recv_sem=rs4.at[q // (NQ - 1)],
            device_id={"pulse": t}, device_id_type=MESH,
        )

    for core in (1, 0):
        for fa in range(core * 8, core * 8 + 8):
            xs = dft([pair(dmid[b * 16 + fa]) for b in range(16)], -1)
            for fb in range(16):
                re, im = xs[fb]
                power[fa + 16 * fb] = ((re * re + im * im) * (1.0 / 256)).astype(BF16)
        for i in NEAR_LAST:
            to_bins(core, i).start()

        @pl.when(lax.rem(q, 2) == 1 - core)
        def _():
            to_bins(core, 0).start()

    drain(send.at[pl.ds(0, 7)], ss1)
    drain(early.at[pl.ds(0, NZ - 1)], ss3)

    @pl.when(k == 0)
    def _():
        drain(comp.at[:, 1], ss2)
        drain(early.at[:, pl.ds(0, 15)], ss6)

    @pl.when(k == 1)
    def _():
        drain(comp.at[:, 1, :, pl.ds(0, 15)], ss2)
        drain(early, ss6)
        drain(cols.at[pl.ds(0, NZ - 1)], ss7)

    own_rows = pltpu.make_async_copy(power.at[pl.ds(q * 8, 8)], rows.at[q], stores)
    own_rows.start()
    outer = NQ - 1

    @pl.when(q == outer)
    def _():
        own_rows.wait()

    @pl.when(q != outer)
    def _():
        drain(rows.at[outer], rs4.at[1])

    edge = pltpu.make_async_remote_copy(
        src_ref=rows.at[outer], dst_ref=halo, send_sem=ss5, recv_sem=rs5,
        device_id={"range": 1 - r}, device_id_type=MESH,
    )
    edge.start()

    @pl.when(q == outer)
    def _():
        drain(rows.at[pl.ds(0, NQ - 1)], rs4.at[0])

    @pl.when(q != outer)
    def _():
        drain(rows.at[pl.ds(0, NQ - 2)], rs4.at[0])
        own_rows.wait()

    edge.wait()
    drain(power.at[pl.ds(0, 8 * (NQ - 1))], ss4)


def band_table():
    gap = np.abs(np.arange(512)[:, None] - (128 + np.arange(256)[None, :]))
    return ((gap > GUARD) & (gap <= GUARD + TRAIN)).astype(np.float32)


def window(rows, halo, band, out_hbm, win, noise, turned, out, done):
    r = lax.axis_index("range")
    right = r.astype(F32)

    def tile(t):
        return rows[t + r * (31 - 2 * t)].astype(F32).reshape(64, 128)

    def place(i, at, x):
        win[i, :, at * 128 : (at + 1) * 128] = x

    beside = halo[...].astype(F32).reshape(64, 128)
    place(0, 0, (beside * right).astype(BF16))
    place(15, 3, (beside * (1.0 - right)).astype(BF16))
    for i in range(16):
        x0, x1 = tile(2 * i).astype(BF16), tile(2 * i + 1).astype(BF16)
        place(i, 1, x0)
        place(i, 2, x1)
        if i > 0:
            place(i - 1, 3, x0)
        if i < 15:
            place(i + 1, 0, x1)
    copies = []
    for part in range(4):
        here = slice(part * 4, part * 4 + 4)
        noise[part] = jnp.dot(win[here].reshape(256, 512), band[...], preferred_element_type=F32)
        for t in range(part * 8, part * 8 + 8):
            i, e = t // 2 - part * 4, t % 2
            level = noise[part, i * 64 : (i + 1) * 64, e * 128 : (e + 1) * 128]
            got = tile(t) / (level * (1.0 / (2 * TRAIN)) + NOISE_FLOOR)
            for f in range(8):
                turned[t, pl.ds(f, 8, stride=8), :] = got[f * 8 : f * 8 + 8]
            out[:, t * 128 : (t + 1) * 128] = turned[t]
        lanes = pl.ds(part * 1024, 1024)
        copies.append(pltpu.make_async_copy(out.at[:, lanes], out_hbm.at[:, lanes], done.at[part]))
        copies[-1].start()
    for copy in copies:
        copy.wait()


def shards(signal, steering, spectrum):
    lanes, twist = lane_tables()
    dma = pltpu.SemaphoreType.DMA
    hbm = pl.BlockSpec(memory_space=pl.ANY)
    scratch = [
        pltpu.VMEM((2, 16, 8, 4096), BF16),
        pltpu.VMEM((2, 32, 64), BF16),
        pltpu.VMEM((2, 8192), F32),
        pltpu.VMEM((2, 256, 256), BF16),
        pltpu.VMEM((2, 64, 128), F32),
        pltpu.VMEM((64, 128), BF16),
        pltpu.VMEM((64, 128), F32),
        pltpu.VMEM((128, 128), F32),
        pltpu.VMEM((2, 512, 128), F32),
        pltpu.VMEM((2, 512, 128), F32),
        pltpu.VMEM((32, 256, 128), F32),
        pltpu.VMEM((8, 8, 4, 32, 128), BF16),
        pltpu.VMEM((8, 8, 4, 32, 128), BF16),
        pltpu.VMEM((2, 8, 64, 128), F32),
        pltpu.VMEM((4, 64, 16, 128), F32),
        pltpu.VMEM((64, 16, 128), F32),
        pltpu.VMEM((512, 256), BF16),
        pltpu.VMEM((512, 256), F32),
        pltpu.VMEM((4, 2, 2, 16, 16, 128), BF16),
        pltpu.VMEM((4, 2, 32, 16, 128), BF16),
        pltpu.VMEM((8, 16, 16, 128), BF16),
        pltpu.VMEM((8, 32, 16, 128), BF16),
        pltpu.VMEM((256, 16, 128), F32),
        pltpu.VMEM((256, 8, 128), BF16),
        dma((4,)), dma((CHUNKS,)),
        dma, dma((CHUNKS,)),
        dma, dma((4,)),
        dma, dma((4,)),
        dma, dma((2,)),
        dma, dma,
        dma, dma,
        dma, dma,
        dma,
    ]
    rows, halo = pl.pallas_call(
        kernel,
        out_shape=[jax.ShapeDtypeStruct((32, 8, 8, 128), BF16), jax.ShapeDtypeStruct((8, 8, 128), BF16)],
        in_specs=[hbm] * 5,
        out_specs=[hbm, hbm],
        scratch_shapes=scratch,
        compiler_params=pltpu.CompilerParams(collective_id=0, has_side_effects=True, vmem_limit_bytes=60 * 2**20),
        name="radar",
    )(signal, steering, spectrum, jnp.asarray(lanes, BF16), jnp.asarray(twist, F32))
    got = pl.pallas_call(
        window,
        out_shape=jax.ShapeDtypeStruct((64, 4096), F32),
        in_specs=[pl.BlockSpec(memory_space=pltpu.VMEM)] * 3,
        out_specs=hbm,
        scratch_shapes=[
            pltpu.VMEM((16, 64, 512), BF16),
            pltpu.VMEM((4, 256, 256), F32),
            pltpu.VMEM((32, 64, 128), F32),
            pltpu.VMEM((64, 4096), F32),
            dma((4,)),
        ],
        compiler_params=pltpu.CompilerParams(vmem_limit_bytes=60 * 2**20),
        name="window",
    )(rows, halo, jnp.asarray(band_table(), BF16))
    return got.reshape(8, 8, 4096)


def solution(mesh):
    return jax.shard_map(
        shards,
        mesh=mesh,
        in_specs=(P(None, "chan", "pulse", "range"), P(), P()),
        out_specs=P("chan", "pulse", "range"),
        check_vma=False,
    )
```
